256 devices in a mesh: grp: 4 (over y), cp: 64 (over x, z, core).
Axes of the slice: x: 4, y: 4, z: 8, core: 2. Of those that a mesh axis runs over, the one named last changes fastest.
Arguments:
- queries: bfloat16 [131072, 2048], P(('grp', 'cp')), parts along dimension 0, may hold values from -6 to 6
- keys: bfloat16 [131072, 1024], P(('grp', 'cp')), parts along dimension 0, may hold values from -8 to 8
- values: bfloat16 [131072, 1024], P(('grp', 'cp')), parts along dimension 0, may hold values from -6 to 6
- doc_lengths: int32 [1024], P('grp'), parts along dimension 0, may hold values from 1 to 1024, 32768 in all
Outputs:
- attended: bfloat16 [131072, 2048], P(('grp', 'cp')), parts along dimension 0
The draws below stay inside these ranges and needn't reach their ends.
There are 4 independent parts, one for each index of `grp`. The reference program is written for one: setup_inputs(seed, part) draws one part's arguments, and reference() takes and returns one part's arrays. A program takes and returns all parts, laid end to end along the dimension named above; each array names one. Nothing has to cross between parts.
Inputs may be any that keep to these rules, and one draw needn't show every extreme that they name: doc_lengths sums to 32768, and its largest entry is exactly 1024.
All inputs are finite; a program needn't handle non-finite values.
Results may differ from the reference program's by a relative error of at most 0.0031.
Values may be sent and summed in bfloat16 or wider, within the bound.
A program may use at most 64 MiB of HBM per device.

```python
import math
import jax
import jax.numpy as jnp
import numpy as np
from jax import lax

HQ = 16
HK = 8
DH = 128
TOK_DEV = 512
REACH = 2
TOKENS = 32768
MAXDOC = 1024
DOCS = 256


def draw_queries(key, part):
    drawn = jnp.clip(jax.random.normal(jax.random.fold_in(key, 11), (TOKENS, HQ * DH), jnp.float32), -6.0, 6.0)
    return drawn.astype(jnp.bfloat16)


def draw_keys(key, part):
    drawn = jnp.clip(jax.random.normal(jax.random.fold_in(key, 22), (TOKENS, HK * DH), jnp.float32), -6.0, 6.0)
    return drawn.astype(jnp.bfloat16)


def shard_levels(rng, extent, shards, low, largest):
    factor_of, own = 1.0, jax.random.fold_in(rng, 6)
    for dim, blocks in shards:
        draws = jnp.exp(jax.random.uniform(jax.random.fold_in(own, dim), (blocks,), jnp.float32, low / len(shards), largest / len(shards)))
        factor_of = factor_of * jnp.repeat(draws, extent[dim] // blocks).reshape([-1 if axis == dim else 1 for axis in range(len(extent))])
    return factor_of


def profile(count, total, bound, skew):
    weights = [(1 << 20) // math.isqrt(standing ** skew) + 1 for standing in range(2, count + 1)]
    surplus, given = total - bound - (count - 1), [1] * (count - 1)
    while surplus > 0:
        movable = [i for i in range(count - 1) if given[i] < bound]
        mass, remaining = sum([weights[i] for i in movable]), surplus
        for i in movable:
            extra = min(bound - given[i], max(1, remaining * weights[i] // mass), surplus)
            given[i] = given[i] + extra
            surplus = surplus - extra
    return np.array([bound] + given)


def ragged_sizes(key, number_of, total, most, skew):
    if number_of == 2:
        one = jax.random.randint(key, (), max(1, total - most), min(most, total - 1) + 1)
        return jnp.stack([one, total - one])
    lengths = jnp.asarray(profile(number_of, total, most, skew), jnp.int32)
    couples = (number_of - 1) // 2
    source_of, taker = lengths[1:1 + 2 * couples:2], lengths[2:2 + 2 * couples:2]
    room = jnp.minimum(source_of - 1, most - taker)
    passed = jax.random.randint(jax.random.fold_in(key, 1), (couples,), 0, 1 << 20) % (room + 1)
    lengths = lengths.at[1:1 + 2 * couples:2].set(source_of - passed).at[2:2 + 2 * couples:2].set(taker + passed)
    return lengths[jax.random.permutation(jax.random.fold_in(key, 2), number_of)]


def noise(rng, dims, spread, limit, shards=(), held_as=jnp.bfloat16):
    loudness = shard_levels(rng, dims, shards, -0.22, 0.18) if shards else 1.0
    array = jax.random.normal(rng, dims, jnp.float32) * spread * loudness
    return jnp.minimum(jnp.maximum(array, -limit), limit).astype(held_as)


def setup_inputs(seed: int = 0, part: int = 0) -> dict:
    arg_keys = jax.random.split(jax.random.key(seed), 5)
    part_splits = jax.random.split(jax.random.fold_in(arg_keys[4], part), 5)
    queries = draw_queries(jax.random.fold_in(jax.random.fold_in(arg_keys[4], part), 71), part)
    keys = draw_keys(jax.random.fold_in(jax.random.fold_in(arg_keys[4], part), 71), part)
    values = noise(part_splits[2], (TOKENS, HK * DH), 1.0, 6.0, ((0, 64),))
    doc_lengths = ragged_sizes(part_splits[3], DOCS, TOKENS, MAXDOC, 2).astype(jnp.int32)
    return {"queries": queries, "keys": keys, "values": values, "doc_lengths": doc_lengths}


query_scale = 144.0 ** -0.5


def doc_index(positions, doc_ends):
    return jnp.sum((positions[:, None] >= doc_ends[None, :]).astype(jnp.int32), axis=1).astype(jnp.int32)


def attend(query_rows, key_rows, value_rows, visible):
    tok_rows = query_rows.shape[0]
    key_count = key_rows.shape[0]
    groups = HQ // HK
    query_heads = query_rows.astype(jnp.float32).reshape(tok_rows, HK, groups, DH)
    key_heads = key_rows.astype(jnp.float32).reshape(key_count, HK, DH)
    value_heads = value_rows.astype(jnp.float32).reshape(key_count, HK, DH)
    scores = jnp.einsum("tkgd,wkd->kgtw", query_heads, key_heads) * query_scale
    scores = jnp.where(visible[None, None], scores, -jnp.inf)
    highest = jnp.max(scores, axis=-1, keepdims=True)
    weights = jnp.exp(scores - highest)
    totals = jnp.sum(weights, axis=-1)
    rounded = lax.optimization_barrier(weights.astype(jnp.bfloat16))
    mixed = jnp.einsum("kgtw,wkd->tkgd", rounded.astype(jnp.float32), value_heads)
    mixed = mixed / jnp.transpose(totals, (2, 0, 1))[..., None]
    return mixed.reshape(tok_rows, HQ * DH).astype(jnp.bfloat16)


def reference(queries, keys, values, doc_lengths):
    doc_ends = jnp.cumsum(doc_lengths).astype(jnp.int32)
    margin = REACH * TOK_DEV
    window = (REACH + 1) * TOK_DEV
    pad_keys = jnp.concatenate([jnp.zeros((margin, HK * DH), keys.dtype), keys], axis=0)
    pad_values = jnp.concatenate([jnp.zeros((margin, HK * DH), values.dtype), values], axis=0)

    def one_block(index):
        begin_row = (index * TOK_DEV).astype(jnp.int32)
        query_pos = begin_row + jnp.arange(TOK_DEV, dtype=jnp.int32)
        key_pos = begin_row - margin + jnp.arange(window, dtype=jnp.int32)
        same_doc = doc_index(query_pos, doc_ends)[:, None] == doc_index(key_pos, doc_ends)[None, :]
        visible = same_doc & (key_pos[None, :] <= query_pos[:, None]) & (key_pos[None, :] >= 0)
        query_rows = lax.dynamic_slice_in_dim(queries, begin_row, TOK_DEV, 0)
        key_rows = lax.dynamic_slice_in_dim(pad_keys, begin_row, window, 0)
        value_rows = lax.dynamic_slice_in_dim(pad_values, begin_row, window, 0)
        return attend(query_rows, key_rows, value_rows, visible)

    blocks = lax.map(one_block, jnp.arange(TOKENS // TOK_DEV, dtype=jnp.int32))
    return blocks.reshape(TOKENS, HQ * DH)
```

```python
import functools
import math

import jax
import jax.numpy as jnp
from jax import lax
from jax.experimental import pallas as pl
from jax.experimental.pallas import tpu as pltpu
from jax.sharding import PartitionSpec as P

DH = 128
T = 512
B = 128
LAG = 2
BIG = 32768.0
NEG = -1e30
SCALE = 144.0 ** (-0.5) * math.log2(math.e)
MESH = pl.DeviceIdType.MESH
F32, BF16, I32 = jnp.float32, jnp.bfloat16, jnp.int32


def stacked(pair):
    return jnp.concatenate([pair[:, :DH], pair[:, DH:]], axis=0)


def unstacked(x):
    return jnp.concatenate([x[:B], x[B:]], axis=1)


def kernel(
    q_hbm, k_hbm, v_hbm, len_ref, o_hbm,
    kv, qv, qr, msg, outv, stat_s, stat_r, augk, augq, augr, flags,
    loc_sem, q_send, q_recv, own_send, own_recv, msg_send, msg_recv,
    st_send, st_recv, fwd_send, fwd_recv, out_sem,
):
    hk = kv.shape[0]
    n = lax.axis_size("cp")
    me = lax.axis_index("cp")
    core = lax.rem(me, 2)
    chip = lax.div(me, 2)
    partner = me + 1 - 2 * core
    after = lax.rem(me + 2, n)
    before = lax.rem(me + n - 2, n)
    own0 = pl.multiple_of(T + T * core, T)
    barrier = pltpu.get_barrier_semaphore()

    def local(h):
        lo = pl.ds(pl.multiple_of(h * DH, DH), DH)
        two = pl.ds(pl.multiple_of(h * 2 * DH, DH), 2 * DH)
        mine = pl.ds(own0, T)
        return (
            pltpu.make_async_copy(k_hbm.at[:, lo], kv.at[h, mine, pl.ds(0, DH)], loc_sem.at[0, h]),
            pltpu.make_async_copy(v_hbm.at[:, lo], kv.at[h, mine, pl.ds(DH, DH)], loc_sem.at[1, h]),
            pltpu.make_async_copy(q_hbm.at[:, two], qv.at[h], loc_sem.at[2, h]),
        )

    def remote(src, dst, send, recv, to):
        return pltpu.make_async_remote_copy(src, dst, send, recv, device_id={"cp": to}, device_id_type=MESH)

    def send_q(h):
        two = pl.ds(pl.multiple_of(h * 2 * DH, DH), 2 * DH)
        return remote(q_hbm.at[:, two], qr.at[h], q_send.at[h], q_recv.at[h], before)

    def send_own(h):
        mine = kv.at[h, pl.ds(own0, T)]
        return remote(mine, mine, own_send.at[h], own_recv.at[h], partner)

    def send_msg(h):
        return remote(msg.at[h], kv.at[h, pl.ds(0, T)], msg_send.at[h], msg_recv.at[h], after)

    def send_stat(h):
        return remote(stat_s.at[h], stat_r.at[h], st_send.at[h], st_recv.at[h], after)

    def forward(h):
        part = kv.at[h, pl.ds(0, T)]
        return remote(part, part, fwd_send.at[h], fwd_recv.at[h], partner)

    def put(h):
        two = pl.ds(pl.multiple_of(h * 2 * DH, DH), 2 * DH)
        return pltpu.make_async_copy(outv.at[h], o_hbm.at[:, two], out_sem.at[h])

    def every(body):
        def step(h, carry):
            body(h)
            return carry

        lax.fori_loop(0, hk, step, 0)

    @pl.when(core == 0)
    def _():
        for other in (before, after, partner):
            pl.semaphore_signal(barrier, inc=1, device_id={"cp": other}, device_id_type=MESH)
        pl.semaphore_wait(barrier, 3)
        every(lambda h: send_q(h).start())

    @pl.when(core == 1)
    def _():
        pl.semaphore_signal(barrier, inc=1, device_id={"cp": partner}, device_id_type=MESH)
        pl.semaphore_wait(barrier, 1)

    def start_local(h):
        for copy in local(h):
            copy.start()

    every(start_local)

    lens = jnp.broadcast_to(len_ref[...], (8, len_ref.shape[1]))
    docs = lens.shape[1]
    upto = lax.broadcasted_iota(I32, (docs, docs), 0) <= lax.broadcasted_iota(I32, (docs, docs), 1)
    upto = jnp.where(upto, 1.0, 0.0).astype(BF16)
    high = lax.shift_right_logical(lens, 5).astype(F32).astype(BF16)
    low = (lens & 31).astype(F32).astype(BF16)
    ends = 32.0 * jnp.dot(high, upto, preferred_element_type=F32) + jnp.dot(low, upto, preferred_element_type=F32)
    ends = ends[0:1].astype(I32)
    ones = jnp.ones((docs, DH), BF16)

    def doc_of(pos):
        past = jnp.where(pos >= ends, 1.0, 0.0).astype(BF16)
        return jnp.dot(past, ones, preferred_element_type=F32)

    def doc_rows(base, rows):
        return doc_of(lax.broadcasted_iota(I32, (rows, docs), 0) + base)

    def doc_at(p):
        return doc_of(jnp.zeros((8, docs), I32) + p)

    def bits(doc):
        lane = lax.broadcasted_iota(I32, doc.shape, 1)
        return (lax.shift_right_logical(doc.astype(I32), lane & 7) & 1).astype(F32), lane

    def key_side(doc, hidden):
        b, lane = bits(doc)
        out = jnp.where(lane < 8, b - 1.0, jnp.where(lane < 16, -b, jnp.where(lane == 16, -hidden, 0.0)))
        return (out * BIG).astype(BF16)

    def query_side(doc):
        b, lane = bits(doc)
        return jnp.where(lane < 8, b, jnp.where(lane < 16, 1.0 - b, jnp.where(lane == 16, 1.0, 0.0))).astype(BF16)

    first = chip * (2 * T)
    inner = jnp.where(chip > 0, 1.0, 0.0)
    far_left = jnp.where(doc_at(first - T - 1) == doc_at(first), 1.0, 0.0) * inner
    far_right = jnp.where(doc_at(first + T - 1) == doc_at(first + 2 * T), 1.0, 0.0)
    flags[0] = far_left
    flags[1] = far_right
    hidden = jnp.maximum(far_left, 1.0 - inner)[0:1]
    for part in range(3):
        doc = doc_rows(first + (part - 1) * T, T)
        augk[part * T : (part + 1) * T] = key_side(doc, hidden if part == 0 else 0.0)
    augq[...] = query_side(doc_rows(me * T, T))
    augr[...] = query_side(doc_rows(first + 2 * T, T))

    ones_v = jnp.ones((3 * T, DH), BF16)
    row = lax.broadcasted_iota(I32, (2 * B, B), 0)
    causal = lax.broadcasted_iota(I32, (2 * B, B), 1) <= (row & (B - 1))

    def scores(h, pair, aug, lo, hi):
        q = jnp.concatenate([stacked(pair), jnp.concatenate([aug, aug], axis=0)], axis=1)
        k = jnp.concatenate([kv[h, lo:hi, 0:DH], augk[lo:hi]], axis=1)
        return lax.dot_general(q, k, (((1,), (1,)), ((), ())), preferred_element_type=F32)

    def mixed(h, s, top, lo, hi):
        p = jnp.exp2(s * SCALE - top).astype(BF16)
        v = jnp.concatenate([kv[h, lo:hi, DH : 2 * DH], ones_v[: hi - lo]], axis=1)
        o = jnp.dot(p, v, preferred_element_type=F32)
        return o[:, :DH], o[:, DH:]

    def masked(s):
        return jnp.concatenate([s[:, :-B], jnp.where(causal, s[:, -B:], NEG)], axis=1)

    def border_block(h, r):
        rows = slice(r * B, (r + 1) * B)
        lo, hi = T + r * B, 3 * T
        s = scores(h, qr[h, rows], augr[rows], lo, hi)
        top = jnp.max(s, axis=1, keepdims=True) * SCALE
        acc, total = mixed(h, s, top, lo, hi)
        partial = unstacked(acc / total)
        own = kv[h, 2 * T + r * B : 2 * T + (r + 1) * B].astype(F32)
        msg[h, rows] = jnp.where(flags[1][0:1, 0:1] > 0.5, partial, own).astype(BF16)
        level = top + jnp.log2(total)
        even = (lax.broadcasted_iota(I32, (B, DH), 1) & 1) == 0
        stat_s[h, :, rows] = jnp.transpose(jnp.where(even, level[:B], level[B:]))[0:8]

    def head_block(h, r):
        rows = slice(r * B, (r + 1) * B)
        hi = T + (r + 1) * B
        s = masked(scores(h, qv[h, rows], augq[rows], 0, hi))
        level = jnp.concatenate(
            [jnp.transpose(jnp.broadcast_to(stat_r[h, i : i + 1, rows], (DH, B))) for i in range(2)], axis=0
        )
        level = jnp.where(flags[0][0:1] > 0.5, level, NEG)
        top = jnp.maximum(jnp.max(s, axis=1, keepdims=True) * SCALE, level[:, 0:1])
        acc, total = mixed(h, s, top, 0, hi)
        weight = jnp.exp2(level - top)
        other = stacked(kv[h, rows]).astype(F32)
        outv[h, rows] = unstacked((acc + weight * other) / (total + weight)).astype(BF16)

    def tail_block(h, r):
        rows = slice(r * B, (r + 1) * B)
        lo, hi = r * B, 2 * T + (r + 1) * B
        s = masked(scores(h, qv[h, rows], augq[rows], lo, hi))
        top = jnp.max(s, axis=1, keepdims=True) * SCALE
        acc, total = mixed(h, s, top, lo, hi)
        outv[h, rows] = unstacked(acc / total).astype(BF16)

    def share(h):
        for copy in local(h):
            copy.wait()
        send_own(h).start()

    every(share)

    @pl.when(core == 0)
    def _():
        def step(it, carry):
            @pl.when(it < hk)
            def _():
                send_q(it).wait_recv()
                send_own(it).wait_recv()
                for r in range(T // B):
                    border_block(it, r)
                send_msg(it).start()
                send_stat(it).start()

            @pl.when(it >= LAG)
            def _():
                h = it - LAG
                send_msg(h).wait_recv()
                send_stat(h).wait_recv()
                forward(h).start()
                for r in range(T // B):
                    head_block(h, r)
                put(h).start()

            return carry

        lax.fori_loop(0, hk + LAG, step, 0)

        def finish(h):
            send_q(h).wait_send()
            send_own(h).wait_send()
            send_msg(h).wait_send()
            send_stat(h).wait_send()
            forward(h).wait_send()
            put(h).wait()

        every(finish)

    @pl.when(core == 1)
    def _():
        def step(h):
            send_own(h).wait_recv()
            forward(h).wait_recv()
            for r in range(T // B):
                tail_block(h, r)
            put(h).start()

        every(step)

        def finish(h):
            send_own(h).wait_send()
            put(h).wait()

        every(finish)


def on_device(queries, keys, values, doc_lengths):
    hk = keys.shape[1] // DH
    docs = doc_lengths.shape[0]
    sem = pltpu.SemaphoreType.DMA
    any_spec = pl.BlockSpec(memory_space=pl.ANY)
    return pl.pallas_call(
        kernel,
        out_shape=jax.ShapeDtypeStruct(queries.shape, BF16),
        in_specs=[any_spec, any_spec, any_spec, pl.BlockSpec(memory_space=pltpu.VMEM)],
        out_specs=any_spec,
        scratch_shapes=[
            pltpu.VMEM((hk, 3 * T, 2 * DH), BF16),
            pltpu.VMEM((hk, T, 2 * DH), BF16),
            pltpu.VMEM((hk, T, 2 * DH), BF16),
            pltpu.VMEM((hk, T, 2 * DH), BF16),
            pltpu.VMEM((hk, T, 2 * DH), BF16),
            pltpu.VMEM((hk, 8, T), F32),
            pltpu.VMEM((hk, 8, T), F32),
            pltpu.VMEM((3 * T, DH), BF16),
            pltpu.VMEM((T, DH), BF16),
            pltpu.VMEM((T, DH), BF16),
            pltpu.VMEM((2, 8, DH), F32),
            sem((3, hk)),
        ]
        + [sem((hk,))] * 11,
        compiler_params=pltpu.CompilerParams(
            collective_id=0, has_side_effects=True, vmem_limit_bytes=60 * 1024 * 1024
        ),
    )(queries, keys, values, doc_lengths.reshape(1, docs))


def solution(mesh):
    return jax.shard_map(
        on_device,
        mesh=mesh,
        in_specs=(P(("grp", "cp"), None), P(("grp", "cp"), None), P(("grp", "cp"), None), P("grp")),
        out_specs=P(("grp", "cp"), None),
        check_vma=False,
    )
```

```python
import functools
import math

import jax
import jax.numpy as jnp
from jax import lax
from jax.experimental import pallas as pl
from jax.experimental.pallas import tpu as pltpu
from jax.sharding import PartitionSpec as P

DH = 128
T = 512
B = 128
LAG = 3
BIG = 32768.0
NEG = -1e30
SCALE = 144.0 ** (-0.5) * math.log2(math.e)
MESH = pl.DeviceIdType.MESH
F32, BF16, I32 = jnp.float32, jnp.bfloat16, jnp.int32


def stacked(pair):
    return jnp.concatenate([pair[:, :DH], pair[:, DH:]], axis=0)


def kernel(
    q_hbm, k_hbm, v_hbm, len_ref, o_hbm,
    kv, qv, qr, raw, msg, outv, stat_s, stat_r, augk, augq, augr, flags,
    loc_sem, q_send, q_recv, own_send, own_recv, msg_send, msg_recv,
    st_send, st_recv, fwd_send, fwd_recv, out_sem,
):
    hk = kv.shape[0]
    n = lax.axis_size("cp")
    me = lax.axis_index("cp")
    core = lax.rem(me, 2)
    chip = lax.div(me, 2)
    partner = me + 1 - 2 * core
    next_head = lax.rem(me + 2 - core, n)
    last_head = lax.rem(me + n - 2, n)
    last_tail = lax.rem(me + n - 1, n)
    own0 = pl.multiple_of(T + T * core, T)
    barrier = pltpu.get_barrier_semaphore()
    half = T // 2

    def lanes(h, width):
        return pl.ds(pl.multiple_of(h * width, DH), width)

    def local(h):
        mine = pl.ds(own0, T)
        return (
            pltpu.make_async_copy(k_hbm.at[:, lanes(h, DH)], kv.at[h, mine, pl.ds(0, DH)], loc_sem.at[0, h]),
            pltpu.make_async_copy(v_hbm.at[:, lanes(h, DH)], raw.at[h], loc_sem.at[1, h]),
            pltpu.make_async_copy(q_hbm.at[:, lanes(h, 2 * DH)], qv.at[h], loc_sem.at[2, h]),
        )

    def remote(src, dst, send, recv, to):
        return pltpu.make_async_remote_copy(src, dst, send, recv, device_id={"cp": to}, device_id_type=MESH)

    def send_q(h, part):
        src = q_hbm.at[pl.ds(part * half, half), lanes(h, 2 * DH)]
        return remote(src, qr.at[h], q_send.at[part, h], q_recv.at[h], (last_head, last_tail)[part])

    def send_own(h):
        mine = kv.at[h, pl.ds(own0, T)]
        return remote(mine, mine, own_send.at[h], own_recv.at[h], partner)

    def send_msg(h, part):
        dst = kv.at[h, pl.ds(part * half, half)]
        return remote(msg.at[h], dst, msg_send.at[h], msg_recv.at[part, h], next_head)

    def send_stat(h, part):
        return remote(stat_s.at[h], stat_r.at[part, h], st_send.at[h], st_recv.at[part, h], next_head)

    def forward(h):
        part = kv.at[h, pl.ds(0, T)]
        return remote(part, part, fwd_send.at[h], fwd_recv.at[h], partner)

    def put(h):
        return pltpu.make_async_copy(outv.at[h], o_hbm.at[:, lanes(h, 2 * DH)], out_sem.at[h])

    def every(body):
        def step(h, carry):
            body(h)
            return carry

        lax.fori_loop(0, hk, step, 0)

    @pl.when(core == 0)
    def _():
        for other in (last_head, last_tail, next_head, partner):
            pl.semaphore_signal(barrier, inc=1, device_id={"cp": other}, device_id_type=MESH)
        pl.semaphore_wait(barrier, 4)

        def start(h):
            send_q(h, 0).start()
            send_q(h, 1).start()

        every(start)

    @pl.when(core == 1)
    def _():
        for other in (next_head, partner):
            pl.semaphore_signal(barrier, inc=1, device_id={"cp": other}, device_id_type=MESH)
        pl.semaphore_wait(barrier, 2)

    def start_local(h):
        for copy in local(h):
            copy.start()

    every(start_local)

    lens = jnp.broadcast_to(len_ref[...], (8, len_ref.shape[1]))
    docs = lens.shape[1]
    upto = lax.broadcasted_iota(I32, (docs, docs), 0) <= lax.broadcasted_iota(I32, (docs, docs), 1)
    upto = jnp.where(upto, 1.0, 0.0).astype(BF16)
    high = lax.shift_right_logical(lens, 5).astype(F32).astype(BF16)
    low = (lens & 31).astype(F32).astype(BF16)
    ends = 32.0 * jnp.dot(high, upto, preferred_element_type=F32) + jnp.dot(low, upto, preferred_element_type=F32)
    ends = ends[0:1].astype(I32)
    ones = jnp.ones((docs, DH), BF16)

    def doc_of(pos):
        past = jnp.where(pos >= ends, 1.0, 0.0).astype(BF16)
        return jnp.dot(past, ones, preferred_element_type=F32)

    def doc_rows(base, rows):
        return doc_of(lax.broadcasted_iota(I32, (rows, docs), 0) + base)

    def doc_at(p):
        return doc_of(jnp.zeros((8, docs), I32) + p)

    def bits(doc):
        lane = lax.broadcasted_iota(I32, doc.shape, 1)
        return (lax.shift_right_logical(doc.astype(I32), lane & 7) & 1).astype(F32), lane

    def key_side(doc, hidden):
        b, lane = bits(doc)
        out = jnp.where(lane < 8, b - 1.0, jnp.where(lane < 16, -b, jnp.where(lane == 16, -hidden, 0.0)))
        return (out * BIG).astype(BF16)

    def query_side(doc):
        b, lane = bits(doc)
        return jnp.where(lane < 8, b, jnp.where(lane < 16, 1.0 - b, jnp.where(lane == 16, 1.0, 0.0))).astype(BF16)

    first = chip * (2 * T)
    inner = jnp.where(chip > 0, 1.0, 0.0)
    far_left = jnp.where(doc_at(first - T - 1) == doc_at(first), 1.0, 0.0) * inner
    far_right = jnp.where(doc_at(first + T - 1) == doc_at(first + 2 * T), 1.0, 0.0)
    flags[0] = far_left
    flags[1] = far_right
    hidden = jnp.maximum(far_left, 1.0 - inner)[0:1]
    for part in range(3):
        doc = doc_rows(first + (part - 1) * T, T)
        augk[part * T : (part + 1) * T] = key_side(doc, hidden if part == 0 else 0.0)
    augq[...] = query_side(doc_rows(me * T, T))
    augr[...] = query_side(doc_rows(first + 2 * T + core * half, half))

    ones_v = jnp.ones((16, 3 * T), BF16)
    column = lax.broadcasted_iota(I32, (B, 2 * B), 1)
    causal = lax.broadcasted_iota(I32, (B, 2 * B), 0) <= (column & (B - 1))

    def scores(h, pair, aug, lo, hi):
        q = jnp.concatenate([stacked(pair), jnp.concatenate([aug, aug], axis=0)], axis=1)
        k = jnp.concatenate([kv[h, lo:hi, 0:DH], augk[lo:hi]], axis=1)
        return lax.dot_general(k, q, (((1,), (1,)), ((), ())), preferred_element_type=F32)

    def mixed(h, s, top, lo, hi):
        p = jnp.exp2(s * SCALE - top).astype(BF16)
        v = jnp.concatenate([kv[h, i : i + B, DH : 2 * DH] for i in range(lo, hi, B)], axis=1)
        v = jnp.concatenate([v, ones_v[:, : hi - lo]], axis=0)
        o = jnp.dot(v, p, preferred_element_type=F32)
        return o[:DH], o[DH : DH + 1]

    def masked(s):
        return jnp.concatenate([s[:-B], jnp.where(causal, s[-B:], NEG)], axis=0)

    def store(h, r, o):
        rows = slice(r * B, (r + 1) * B)
        outv[h, rows, 0:DH] = jnp.transpose(o[:, :B]).astype(BF16)
        outv[h, rows, DH : 2 * DH] = jnp.transpose(o[:, B:]).astype(BF16)

    def border_block(h, i, part):
        rows = slice(i * B, (i + 1) * B)
        r = part * 2 + i
        lo, hi = T + r * B, 3 * T
        s = scores(h, qr[h, rows], augr[rows], lo, hi)
        top = jnp.max(s, axis=0, keepdims=True) * SCALE
        acc, total = mixed(h, s, top, lo, hi)
        own = kv[h, 2 * T + r * B : 2 * T + (r + 1) * B].astype(F32)
        msg[h, rows] = jnp.where(flags[1][0:1, 0:1] > 0.5, acc / total, own).astype(BF16)
        stat_s[h, i : i + 1] = top + jnp.log2(total)

    def border(h, part):
        send_q(h, part).wait_recv()
        send_own(h).wait_recv()
        for i in range(2):
            border_block(h, i, part)
        send_msg(h, part).start()
        send_stat(h, part).start()

    def head_block(h, r):
        rows = slice(r * B, (r + 1) * B)
        hi = T + (r + 1) * B
        s = masked(scores(h, qv[h, rows], augq[rows], 0, hi))
        level = jnp.where(flags[0][0:1, 0:1] > 0.5, stat_r[r // 2, h, r % 2 : r % 2 + 1], NEG)
        top = jnp.maximum(jnp.max(s, axis=0, keepdims=True) * SCALE, level)
        acc, total = mixed(h, s, top, 0, hi)
        weight = jnp.exp2(level - top)
        store(h, r, (acc + weight * kv[h, rows].astype(F32)) / (total + weight))

    def tail_block(h, r):
        rows = slice(r * B, (r + 1) * B)
        lo, hi = r * B, 2 * T + (r + 1) * B
        s = masked(scores(h, qv[h, rows], augq[rows], lo, hi))
        top = jnp.max(s, axis=0, keepdims=True) * SCALE
        acc, total = mixed(h, s, top, lo, hi)
        store(h, r, acc / total)

    def turn(h):
        for copy in local(h):
            copy.wait()
        for i in range(T // B):
            block = jnp.transpose(raw[h, i * B : (i + 1) * B].astype(F32)).astype(BF16)
            kv[h, pl.ds(pl.multiple_of(own0 + i * B, B), B), DH : 2 * DH] = block

    def share(h):
        @pl.when(h < hk)
        def _():
            turn(h)

        @pl.when(h > 0)
        def _():
            send_own(h - 1).start()

    def share_step(h, carry):
        share(h)
        return carry

    lax.fori_loop(0, hk + 1, share_step, 0)

    @pl.when(core == 0)
    def _():
        def step(it, carry):
            h = it - LAG

            @pl.when(it >= LAG)
            def _():
                for part in range(2):
                    send_msg(h, part).wait_recv()
                    send_stat(h, part).wait_recv()
                forward(h).start()

            @pl.when(it < hk)
            def _():
                border(it, 0)

            @pl.when(it >= LAG)
            def _():
                for r in range(T // B):
                    head_block(h, r)
                put(h).start()

            return carry

        lax.fori_loop(0, hk + LAG, step, 0)

        def finish(h):
            for part in range(2):
                send_q(h, part).wait_send()
            send_own(h).wait_send()
            send_msg(h, 0).wait_send()
            send_stat(h, 0).wait_send()
            forward(h).wait_send()
            put(h).wait()

        every(finish)

    @pl.when(core == 1)
    def _():
        def step(it, carry):
            h = it - LAG

            @pl.when(it < hk)
            def _():
                border(it, 1)

            @pl.when(it >= LAG)
            def _():
                forward(h).wait_recv()
                for r in range(T // B):
                    tail_block(h, r)
                put(h).start()

            return carry

        lax.fori_loop(0, hk + LAG, step, 0)

        def finish(h):
            send_own(h).wait_send()
            send_msg(h, 1).wait_send()
            send_stat(h, 1).wait_send()
            put(h).wait()

        every(finish)


def on_device(queries, keys, values, doc_lengths):
    hk = keys.shape[1] // DH
    docs = doc_lengths.shape[0]
    sem = pltpu.SemaphoreType.DMA
    any_spec = pl.BlockSpec(memory_space=pl.ANY)
    return pl.pallas_call(
        kernel,
        out_shape=jax.ShapeDtypeStruct(queries.shape, BF16),
        in_specs=[any_spec, any_spec, any_spec, pl.BlockSpec(memory_space=pltpu.VMEM)],
        out_specs=any_spec,
        scratch_shapes=[
            pltpu.VMEM((hk, 3 * T, 2 * DH), BF16),
            pltpu.VMEM((hk, T, 2 * DH), BF16),
            pltpu.VMEM((hk, T // 2, 2 * DH), BF16),
            pltpu.VMEM((hk, T, DH), BF16),
            pltpu.VMEM((hk, T // 2, 2 * DH), BF16),
            pltpu.VMEM((hk, T, 2 * DH), BF16),
            pltpu.VMEM((hk, 8, 2 * B), F32),
            pltpu.VMEM((2, hk, 8, 2 * B), F32),
            pltpu.VMEM((3 * T, DH), BF16),
            pltpu.VMEM((T, DH), BF16),
            pltpu.VMEM((T // 2, DH), BF16),
            pltpu.VMEM((2, 8, DH), F32),
            sem((3, hk)),
            sem((2, hk)),
            sem((hk,)),
            sem((hk,)),
            sem((hk,)),
            sem((hk,)),
            sem((2, hk)),
            sem((hk,)),
            sem((2, hk)),
            sem((hk,)),
            sem((hk,)),
            sem((hk,)),
        ],
        compiler_params=pltpu.CompilerParams(
            collective_id=0, has_side_effects=True, vmem_limit_bytes=60 * 1024 * 1024
        ),
    )(queries, keys, values, doc_lengths.reshape(1, docs))


def solution(mesh):
    return jax.shard_map(
        on_device,
        mesh=mesh,
        in_specs=(P(("grp", "cp"), None), P(("grp", "cp"), None), P(("grp", "cp"), None), P("grp")),
        out_specs=P(("grp", "cp"), None),
        check_vma=False,
    )
```

```python
import functools
import math

import jax
import jax.numpy as jnp
from jax import lax
from jax.experimental import pallas as pl
from jax.experimental.pallas import tpu as pltpu
from jax.sharding import PartitionSpec as P

DH = 128
T = 512
B = 128
LAG = 3
BIG = 32768.0
NEG = -1e30
SCALE = 144.0 ** (-0.5) * math.log2(math.e)
MESH = pl.DeviceIdType.MESH
F32, BF16, I32 = jnp.float32, jnp.bfloat16, jnp.int32


def stacked(pair):
    return jnp.concatenate([pair[:, :DH], pair[:, DH:]], axis=0)


def unstacked(x):
    return jnp.concatenate([x[:B], x[B:]], axis=1)


def kernel(
    q_hbm, k_hbm, v_hbm, len_ref, o_ref,
    kv, qv, qr, msg, stat_s, stat_r, augk, augq, augr, flags,
    loc_sem, q_send, q_recv, own_send, own_recv, msg_send, msg_recv,
    st_send, st_recv, fwd_send, fwd_recv,
):
    hk = kv.shape[0]
    n = lax.axis_size("cp")
    me = lax.axis_index("cp")
    core = lax.rem(me, 2)
    chip = lax.div(me, 2)
    partner = me + 1 - 2 * core
    next_head = lax.rem(me + 2 - core, n)
    last_head = lax.rem(me + n - 2, n)
    last_tail = lax.rem(me + n - 1, n)
    own0 = pl.multiple_of(T + T * core, T)
    barrier = pltpu.get_barrier_semaphore()
    half = T // 2

    def lanes(h, width):
        return pl.ds(pl.multiple_of(h * width, DH), width)

    def local(h):
        mine = pl.ds(own0, T)
        return (
            pltpu.make_async_copy(k_hbm.at[:, lanes(h, DH)], kv.at[h, mine, pl.ds(0, DH)], loc_sem.at[0, h]),
            pltpu.make_async_copy(v_hbm.at[:, lanes(h, DH)], kv.at[h, mine, pl.ds(DH, DH)], loc_sem.at[1, h]),
            pltpu.make_async_copy(q_hbm.at[:, lanes(h, 2 * DH)], qv.at[h], loc_sem.at[2, h]),
        )

    def remote(src, dst, send, recv, to):
        return pltpu.make_async_remote_copy(src, dst, send, recv, device_id={"cp": to}, device_id_type=MESH)

    def send_q(h, part):
        src = q_hbm.at[pl.ds(part * half, half), lanes(h, 2 * DH)]
        return remote(src, qr.at[h], q_send.at[part, h], q_recv.at[h], (last_head, last_tail)[part])

    def send_own(h):
        mine = kv.at[h, pl.ds(own0, T)]
        return remote(mine, mine, own_send.at[h], own_recv.at[h], partner)

    def send_msg(h, part):
        dst = kv.at[h, pl.ds(part * half, half)]
        return remote(msg.at[h], dst, msg_send.at[h], msg_recv.at[part, h], next_head)

    def send_stat(h, part):
        return remote(stat_s.at[h], stat_r.at[part, h], st_send.at[h], st_recv.at[part, h], next_head)

    def forward(h):
        part = kv.at[h, pl.ds(0, T)]
        return remote(part, part, fwd_send.at[h], fwd_recv.at[h], partner)

    def every(body):
        def step(h, carry):
            body(h)
            return carry

        lax.fori_loop(0, hk, step, 0)

    @pl.when(core == 0)
    def _():
        for other in (last_head, last_tail, next_head, partner):
            pl.semaphore_signal(barrier, inc=1, device_id={"cp": other}, device_id_type=MESH)
        pl.semaphore_wait(barrier, 4)

        def start(h):
            send_q(h, 0).start()
            send_q(h, 1).start()

        every(start)

    @pl.when(core == 1)
    def _():
        for other in (next_head, partner):
            pl.semaphore_signal(barrier, inc=1, device_id={"cp": other}, device_id_type=MESH)
        pl.semaphore_wait(barrier, 2)

    def start_local(h):
        for copy in local(h):
            copy.start()

    every(start_local)

    lens = jnp.broadcast_to(len_ref[...], (8, len_ref.shape[1]))
    docs = lens.shape[1]
    upto = lax.broadcasted_iota(I32, (docs, docs), 0) <= lax.broadcasted_iota(I32, (docs, docs), 1)
    upto = jnp.where(upto, 1.0, 0.0).astype(BF16)
    high = lax.shift_right_logical(lens, 5).astype(F32).astype(BF16)
    low = (lens & 31).astype(F32).astype(BF16)
    ends = 32.0 * jnp.dot(high, upto, preferred_element_type=F32) + jnp.dot(low, upto, preferred_element_type=F32)
    ends = ends[0:1].astype(I32)
    ones = jnp.ones((docs, DH), BF16)

    def doc_of(pos):
        past = jnp.where(pos >= ends, 1.0, 0.0).astype(BF16)
        return jnp.dot(past, ones, preferred_element_type=F32)

    def doc_rows(base, rows):
        return doc_of(lax.broadcasted_iota(I32, (rows, docs), 0) + base)

    def doc_at(p):
        return doc_of(jnp.zeros((8, docs), I32) + p)

    def bits(doc):
        lane = lax.broadcasted_iota(I32, doc.shape, 1)
        return (lax.shift_right_logical(doc.astype(I32), lane & 7) & 1).astype(F32), lane

    def key_side(doc, hidden):
        b, lane = bits(doc)
        out = jnp.where(lane < 8, b - 1.0, jnp.where(lane < 16, -b, jnp.where(lane == 16, -hidden, 0.0)))
        return (out * BIG).astype(BF16)

    def query_side(doc):
        b, lane = bits(doc)
        return jnp.where(lane < 8, b, jnp.where(lane < 16, 1.0 - b, jnp.where(lane == 16, 1.0, 0.0))).astype(BF16)

    first = chip * (2 * T)
    inner = jnp.where(chip > 0, 1.0, 0.0)
    far_left = jnp.where(doc_at(first - T - 1) == doc_at(first), 1.0, 0.0) * inner
    far_right = jnp.where(doc_at(first + T - 1) == doc_at(first + 2 * T), 1.0, 0.0)
    flags[0] = far_left
    flags[1] = far_right
    hidden = jnp.maximum(far_left, 1.0 - inner)[0:1]
    for part in range(3):
        doc = doc_rows(first + (part - 1) * T, T)
        augk[part * T : (part + 1) * T] = key_side(doc, hidden if part == 0 else 0.0)
    augq[...] = query_side(doc_rows(me * T, T))
    augr[...] = query_side(doc_rows(first + 2 * T + core * half, half))

    ones_v = jnp.ones((3 * T, DH), BF16)
    row = lax.broadcasted_iota(I32, (2 * B, B), 0)
    causal = lax.broadcasted_iota(I32, (2 * B, B), 1) <= (row & (B - 1))

    def scores(h, pair, aug, lo, hi):
        q = jnp.concatenate([stacked(pair), jnp.concatenate([aug, aug], axis=0)], axis=1)
        k = jnp.concatenate([kv[h, lo:hi, 0:DH], augk[lo:hi]], axis=1)
        return lax.dot_general(q, k, (((1,), (1,)), ((), ())), preferred_element_type=F32)

    def mixed(h, s, top, lo, hi):
        p = jnp.exp2(s * SCALE - top).astype(BF16)
        v = jnp.concatenate([kv[h, lo:hi, DH : 2 * DH], ones_v[: hi - lo]], axis=1)
        o = jnp.dot(p, v, preferred_element_type=F32)
        return o[:, :DH], o[:, DH:]

    def masked(s):
        return jnp.concatenate([s[:, :-B], jnp.where(causal, s[:, -B:], NEG)], axis=1)

    def border_block(h, i, part):
        rows = slice(i * B, (i + 1) * B)
        r = part * 2 + i
        lo, hi = T + r * B, 3 * T
        s = scores(h, qr[h, rows], augr[rows], lo, hi)
        top = jnp.max(s, axis=1, keepdims=True) * SCALE
        acc, total = mixed(h, s, top, lo, hi)
        own = kv[h, 2 * T + r * B : 2 * T + (r + 1) * B].astype(F32)
        msg[h, rows] = jnp.where(flags[1][0:1, 0:1] > 0.5, unstacked(acc / total), own).astype(BF16)
        level = top + jnp.log2(total)
        even = (lax.broadcasted_iota(I32, (B, DH), 1) & 1) == 0
        stat_s[h, :, rows] = jnp.transpose(jnp.where(even, level[:B], level[B:]))[0:8]

    def border(h, part):
        send_q(h, part).wait_recv()
        send_own(h).wait_recv()
        for i in range(2):
            border_block(h, i, part)
        send_msg(h, part).start()
        send_stat(h, part).start()

    def head_block(h, r):
        rows = slice(r * B, (r + 1) * B)
        hi = T + (r + 1) * B
        s = masked(scores(h, qv[h, rows], augq[rows], 0, hi))
        part, at = r // 2, slice((r % 2) * B, (r % 2 + 1) * B)
        level = jnp.concatenate(
            [jnp.transpose(jnp.broadcast_to(stat_r[part, h, i : i + 1, at], (DH, B))) for i in range(2)], axis=0
        )
        level = jnp.where(flags[0][0:1] > 0.5, level, NEG)
        top = jnp.maximum(jnp.max(s, axis=1, keepdims=True) * SCALE, level[:, 0:1])
        acc, total = mixed(h, s, top, 0, hi)
        weight = jnp.exp2(level - top)
        other = stacked(kv[h, rows]).astype(F32)
        o_ref[rows, lanes(h, 2 * DH)] = unstacked((acc + weight * other) / (total + weight)).astype(BF16)

    def tail_block(h, r):
        rows = slice(r * B, (r + 1) * B)
        lo, hi = r * B, 2 * T + (r + 1) * B
        s = masked(scores(h, qv[h, rows], augq[rows], lo, hi))
        top = jnp.max(s, axis=1, keepdims=True) * SCALE
        acc, total = mixed(h, s, top, lo, hi)
        o_ref[rows, lanes(h, 2 * DH)] = unstacked(acc / total).astype(BF16)

    def share(h):
        for copy in local(h):
            copy.wait()
        send_own(h).start()

    every(share)

    @pl.when(core == 0)
    def _():
        def step(it, carry):
            h = it - LAG

            @pl.when(it >= LAG)
            def _():
                for part in range(2):
                    send_msg(h, part).wait_recv()
                    send_stat(h, part).wait_recv()
                forward(h).start()

            @pl.when(it < hk)
            def _():
                border(it, 0)

            @pl.when(it >= LAG)
            def _():
                for r in range(T // B):
                    head_block(h, r)

            return carry

        lax.fori_loop(0, hk + LAG, step, 0)

        def finish(h):
            for part in range(2):
                send_q(h, part).wait_send()
            send_own(h).wait_send()
            send_msg(h, 0).wait_send()
            send_stat(h, 0).wait_send()
            forward(h).wait_send()

        every(finish)

    @pl.when(core == 1)
    def _():
        def step(it, carry):
            h = it - LAG

            @pl.when(it < hk)
            def _():
                border(it, 1)

            @pl.when(it >= LAG)
            def _():
                forward(h).wait_recv()
                for r in range(T // B):
                    tail_block(h, r)

            return carry

        lax.fori_loop(0, hk + LAG, step, 0)

        def finish(h):
            send_own(h).wait_send()
            send_msg(h, 1).wait_send()
            send_stat(h, 1).wait_send()

        every(finish)


def on_device(queries, keys, values, doc_lengths):
    hk = keys.shape[1] // DH
    docs = doc_lengths.shape[0]
    sem = pltpu.SemaphoreType.DMA
    hbm = pl.BlockSpec(memory_space=pltpu.HBM)
    vmem = pl.BlockSpec(memory_space=pltpu.VMEM)
    return pl.pallas_call(
        kernel,
        out_shape=pltpu.VMEM(queries.shape, BF16),
        in_specs=[hbm, hbm, hbm, vmem],
        out_specs=vmem,
        scratch_shapes=[
            pltpu.VMEM((hk, 3 * T, 2 * DH), BF16),
            pltpu.VMEM((hk, T, 2 * DH), BF16),
            pltpu.VMEM((hk, T // 2, 2 * DH), BF16),
            pltpu.VMEM((hk, T // 2, 2 * DH), BF16),
            pltpu.VMEM((hk, 8, 2 * B), F32),
            pltpu.VMEM((2, hk, 8, 2 * B), F32),
            pltpu.VMEM((3 * T, DH), BF16),
            pltpu.VMEM((T, DH), BF16),
            pltpu.VMEM((T // 2, DH), BF16),
            pltpu.VMEM((2, 8, DH), F32),
            sem((3, hk)),
            sem((2, hk)),
            sem((hk,)),
            sem((hk,)),
            sem((hk,)),
            sem((hk,)),
            sem((2, hk)),
            sem((hk,)),
            sem((2, hk)),
            sem((hk,)),
            sem((hk,)),
        ],
        compiler_params=pltpu.CompilerParams(
            collective_id=0, has_side_effects=True, vmem_limit_bytes=30 * 1024 * 1024
        ),
    )(*[pltpu.with_memory_space_constraint(x, pltpu.HBM) for x in (queries, keys, values, doc_lengths.reshape(1, docs))])


def solution(mesh):
    return jax.shard_map(
        on_device,
        mesh=mesh,
        in_specs=(P(("grp", "cp"), None), P(("grp", "cp"), None), P(("grp", "cp"), None), P("grp")),
        out_specs=P(("grp", "cp"), None),
        check_vma=False,
    )
```

```python
import functools
import math

import jax
import jax.numpy as jnp
from jax import lax
from jax.experimental import pallas as pl
from jax.experimental.pallas import tpu as pltpu
from jax.sharding import PartitionSpec as P

DH = 128
T = 512
B = 128
LAG = 5
BIG = 32768.0
NEG = -1e30
SCALE = 144.0 ** (-0.5) * math.log2(math.e)
MESH = pl.DeviceIdType.MESH
F32, BF16, I32 = jnp.float32, jnp.bfloat16, jnp.int32


def stacked(pair):
    return jnp.concatenate([pair[:, :DH], pair[:, DH:]], axis=0)


def kernel(
    q_hbm, k_hbm, v_hbm, len_ref, o_ref,
    kv, qv, qr, raw, msg, stat_s, stat_r, augk, augq, augr, flags,
    loc_sem, q_send, q_recv, own_send, own_recv, msg_send, msg_recv,
    st_send, st_recv, fwd_send, fwd_recv,
):
    hk = kv.shape[0]
    n = lax.axis_size("cp")
    me = lax.axis_index("cp")
    core = lax.rem(me, 2)
    chip = lax.div(me, 2)
    partner = me + 1 - 2 * core
    next_head = lax.rem(me + 2 - core, n)
    last_head = lax.rem(me + n - 2, n)
    last_tail = lax.rem(me + n - 1, n)
    own0 = pl.multiple_of(T + T * core, T)
    barrier = pltpu.get_barrier_semaphore()
    half = T // 2

    def lanes(h, width):
        return pl.ds(pl.multiple_of(h * width, DH), width)

    def local(h):
        mine = pl.ds(own0, T)
        return (
            pltpu.make_async_copy(k_hbm.at[:, lanes(h, DH)], kv.at[h, mine, pl.ds(0, DH)], loc_sem.at[0, h]),
            pltpu.make_async_copy(v_hbm.at[:, lanes(h, DH)], raw.at[h], loc_sem.at[1, h]),
            pltpu.make_async_copy(q_hbm.at[:, lanes(h, 2 * DH)], qv.at[h], loc_sem.at[2, h]),
        )

    def remote(src, dst, send, recv, to):
        return pltpu.make_async_remote_copy(src, dst, send, recv, device_id={"cp": to}, device_id_type=MESH)

    def send_q(h, part):
        src = q_hbm.at[pl.ds(part * half, half), lanes(h, 2 * DH)]
        return remote(src, qr.at[h], q_send.at[part, h], q_recv.at[h], (last_head, last_tail)[part])

    def send_own(h):
        mine = kv.at[h, pl.ds(own0, T)]
        return remote(mine, mine, own_send.at[h], own_recv.at[h], partner)

    def send_msg(h, part):
        dst = kv.at[h, pl.ds(part * half, half)]
        return remote(msg.at[h], dst, msg_send.at[h], msg_recv.at[part, h], next_head)

    def send_stat(h, part):
        return remote(stat_s.at[h], stat_r.at[part, h], st_send.at[h], st_recv.at[part, h], next_head)

    def forward(h):
        part = kv.at[h, pl.ds(0, T)]
        return remote(part, part, fwd_send.at[h], fwd_recv.at[h], partner)

    def every(body):
        def step(h, carry):
            body(h)
            return carry

        lax.fori_loop(0, hk, step, 0)

    has_left = chip > 0
    has_right = chip < lax.div(n, 2) - 1

    def greet(other):
        pl.semaphore_signal(barrier, inc=1, device_id={"cp": other}, device_id_type=MESH)

    greet(partner)

    @pl.when(has_right)
    def _():
        greet(next_head)

    @pl.when(has_left & (core == 0))
    def _():
        greet(last_head)
        greet(last_tail)

    right, left = jnp.where(has_right, 1, 0), jnp.where(has_left, 1, 0)
    pl.semaphore_wait(barrier, 1 + right + 2 * left * (1 - core))

    @pl.when(has_left & (core == 0))
    def _():
        def start(h):
            send_q(h, 0).start()
            send_q(h, 1).start()

        every(start)

    def start_local(h):
        for copy in local(h):
            copy.start()

    every(start_local)

    @pl.when(chip == 0)
    def _():
        def clear(h):
            kv[h, 0:T] = jnp.zeros((T, 2 * DH), BF16)

        every(clear)

    lens = jnp.broadcast_to(len_ref[...], (8, len_ref.shape[1]))
    docs = lens.shape[1]
    upto = lax.broadcasted_iota(I32, (docs, docs), 0) <= lax.broadcasted_iota(I32, (docs, docs), 1)
    upto = jnp.where(upto, 1.0, 0.0).astype(BF16)
    high = lax.shift_right_logical(lens, 5).astype(F32).astype(BF16)
    low = (lens & 31).astype(F32).astype(BF16)
    ends = 32.0 * jnp.dot(high, upto, preferred_element_type=F32) + jnp.dot(low, upto, preferred_element_type=F32)
    ends = ends[0:1].astype(I32)
    ones = jnp.ones((docs, DH), BF16)

    def doc_of(pos):
        past = jnp.where(pos >= ends, 1.0, 0.0).astype(BF16)
        return jnp.dot(past, ones, preferred_element_type=F32)

    def doc_rows(base, rows):
        return doc_of(lax.broadcasted_iota(I32, (rows, docs), 0) + base)

    def doc_at(p):
        return doc_of(jnp.zeros((8, docs), I32) + p)

    def bits(doc):
        lane = lax.broadcasted_iota(I32, doc.shape, 1)
        return (lax.shift_right_logical(doc.astype(I32), lane & 7) & 1).astype(F32), lane

    def key_side(doc, hidden):
        b, lane = bits(doc)
        out = jnp.where(lane < 8, b - 1.0, jnp.where(lane < 16, -b, jnp.where(lane == 16, -hidden, 0.0)))
        return (out * BIG).astype(BF16)

    def query_side(doc):
        b, lane = bits(doc)
        return jnp.where(lane < 8, b, jnp.where(lane < 16, 1.0 - b, jnp.where(lane == 16, 1.0, 0.0))).astype(BF16)

    first = chip * (2 * T)
    inner = jnp.where(chip > 0, 1.0, 0.0)
    far_left = jnp.where(doc_at(first - T - 1) == doc_at(first), 1.0, 0.0) * inner
    far_right = jnp.where(doc_at(first + T - 1) == doc_at(first + 2 * T), 1.0, 0.0)
    flags[0] = far_left
    flags[1] = far_right
    hidden = jnp.maximum(far_left, 1.0 - inner)[0:1]
    for part in range(3):
        doc = doc_rows(first + (part - 1) * T, T)
        augk[part * T : (part + 1) * T] = key_side(doc, hidden if part == 0 else 0.0)
    augq[...] = query_side(doc_rows(me * T, T))
    augr[...] = query_side(doc_rows(first + 2 * T + core * half, half))

    ones_v = jnp.ones((16, 3 * T), BF16)
    column = lax.broadcasted_iota(I32, (B, 2 * B), 1)
    causal = lax.broadcasted_iota(I32, (B, 2 * B), 0) <= (column & (B - 1))

    def scores(h, pair, aug, lo, hi):
        q = jnp.concatenate([stacked(pair), jnp.concatenate([aug, aug], axis=0)], axis=1)
        k = jnp.concatenate([kv[h, lo:hi, 0:DH], augk[lo:hi]], axis=1)
        return lax.dot_general(k, q, (((1,), (1,)), ((), ())), preferred_element_type=F32)

    def mixed(h, s, top, lo, hi):
        p = jnp.exp2(s * SCALE - top).astype(BF16)
        v = jnp.concatenate([kv[h, i : i + B, DH : 2 * DH] for i in range(lo, hi, B)], axis=1)
        v = jnp.concatenate([v, ones_v[:, : hi - lo]], axis=0)
        o = jnp.dot(v, p, preferred_element_type=F32)
        return o[:DH], o[DH : DH + 1]

    def masked(s):
        return jnp.concatenate([s[:-B], jnp.where(causal, s[-B:], NEG)], axis=0)

    def store(h, r, o):
        rows = slice(r * B, (r + 1) * B)
        o_ref[rows, lanes(2 * h, DH)] = jnp.transpose(o[:, :B]).astype(BF16)
        o_ref[rows, lanes(2 * h + 1, DH)] = jnp.transpose(o[:, B:]).astype(BF16)

    def staggered(blocks):
        ahead = None
        for block in [*blocks, None]:
            if block is not None:
                next(block)
            if ahead is not None:
                next(ahead, None)
            ahead = block

    def border_block(h, i, part):
        rows = slice(i * B, (i + 1) * B)
        r = part * 2 + i
        lo, hi = T + r * B, 3 * T
        s = scores(h, qr[h, rows], augr[rows], lo, hi)
        yield
        top = jnp.max(s, axis=0, keepdims=True) * SCALE
        acc, total = mixed(h, s, top, lo, hi)
        own = kv[h, 2 * T + r * B : 2 * T + (r + 1) * B].astype(F32)
        msg[h, rows] = jnp.where(flags[1][0:1, 0:1] > 0.5, acc / total, own).astype(BF16)
        stat_s[h, i : i + 1] = top + jnp.log2(total)

    def border(h, part):
        send_q(h, part).wait_recv()
        staggered(border_block(h, i, part) for i in range(2))
        send_msg(h, part).start()
        send_stat(h, part).start()

    def head_block(h, r):
        rows = slice(r * B, (r + 1) * B)
        hi = T + (r + 1) * B
        s = masked(scores(h, qv[h, rows], augq[rows], 0, hi))
        yield
        level = jnp.where(flags[0][0:1, 0:1] > 0.5, stat_r[r // 2, h, r % 2 : r % 2 + 1], NEG)
        top = jnp.maximum(jnp.max(s, axis=0, keepdims=True) * SCALE, level)
        acc, total = mixed(h, s, top, 0, hi)
        weight = jnp.exp2(level - top)
        store(h, r, (acc + weight * kv[h, rows].astype(F32)) / (total + weight))

    def tail_block(h, r):
        rows = slice(r * B, (r + 1) * B)
        lo, hi = r * B, 2 * T + (r + 1) * B
        s = masked(scores(h, qv[h, rows], augq[rows], lo, hi))
        yield
        top = jnp.max(s, axis=0, keepdims=True) * SCALE
        acc, total = mixed(h, s, top, lo, hi)
        store(h, r, acc / total)

    def turn(h):
        for copy in local(h):
            copy.wait()
        for i in range(0, T, DH):
            block = jnp.transpose(raw[h, i : i + DH].astype(F32)).astype(BF16)
            kv[h, pl.ds(pl.multiple_of(own0 + i, DH), DH), DH : 2 * DH] = block

    def share(h, carry):
        @pl.when(h < hk)
        def _():
            turn(h)

        @pl.when(h > 0)
        def _():
            send_own(h - 1).start()

        return carry

    lax.fori_loop(0, hk + 1, share, 0)

    @pl.when(core == 0)
    def _():
        def step(it, carry):
            h = it - LAG

            @pl.when((it >= LAG) & has_left)
            def _():
                for part in range(2):
                    send_msg(h, part).wait_recv()
                    send_stat(h, part).wait_recv()
                forward(h).start()

            @pl.when(it < hk)
            def _():
                send_own(it).wait_recv()

                @pl.when(has_right)
                def _():
                    border(it, 0)

            @pl.when(it >= LAG)
            def _():
                staggered(head_block(h, r) for r in range(T // B))

            return carry

        lax.fori_loop(0, hk + LAG, step, 0)

        def finish(h):
            send_own(h).wait_send()

            @pl.when(has_left)
            def _():
                for part in range(2):
                    send_q(h, part).wait_send()
                forward(h).wait_send()

            @pl.when(has_right)
            def _():
                send_msg(h, 0).wait_send()
                send_stat(h, 0).wait_send()

        every(finish)

    @pl.when(core == 1)
    def _():
        def step(it, carry):
            h = it - LAG

            @pl.when(it < hk)
            def _():
                send_own(it).wait_recv()

                @pl.when(has_right)
                def _():
                    border(it, 1)

            @pl.when(it >= LAG)
            def _():
                @pl.when(has_left)
                def _():
                    forward(h).wait_recv()

                staggered(tail_block(h, r) for r in range(T // B))

            return carry

        lax.fori_loop(0, hk + LAG, step, 0)

        def finish(h):
            send_own(h).wait_send()

            @pl.when(has_right)
            def _():
                send_msg(h, 1).wait_send()
                send_stat(h, 1).wait_send()

        every(finish)


def on_device(queries, keys, values, doc_lengths):
    hk = keys.shape[1] // DH
    docs = doc_lengths.shape[0]
    sem = pltpu.SemaphoreType.DMA
    hbm = pl.BlockSpec(memory_space=pltpu.HBM)
    vmem = pl.BlockSpec(memory_space=pltpu.VMEM)
    return pl.pallas_call(
        kernel,
        out_shape=pltpu.VMEM(queries.shape, BF16),
        in_specs=[hbm, hbm, hbm, vmem],
        out_specs=vmem,
        scratch_shapes=[
            pltpu.VMEM((hk, 3 * T, 2 * DH), BF16),
            pltpu.VMEM((hk, T, 2 * DH), BF16),
            pltpu.VMEM((hk, T // 2, 2 * DH), BF16),
            pltpu.VMEM((hk, T, DH), BF16),
            pltpu.VMEM((hk, T // 2, 2 * DH), BF16),
            pltpu.VMEM((hk, 8, 2 * B), F32),
            pltpu.VMEM((2, hk, 8, 2 * B), F32),
            pltpu.VMEM((3 * T, DH), BF16),
            pltpu.VMEM((T, DH), BF16),
            pltpu.VMEM((T // 2, DH), BF16),
            pltpu.VMEM((2, 8, DH), F32),
            sem((3, hk)),
            sem((2, hk)),
            sem((hk,)),
            sem((hk,)),
            sem((hk,)),
            sem((hk,)),
            sem((2, hk)),
            sem((hk,)),
            sem((2, hk)),
            sem((hk,)),
            sem((hk,)),
        ],
        compiler_params=pltpu.CompilerParams(
            collective_id=0, has_side_effects=True, vmem_limit_bytes=30 * 1024 * 1024
        ),
    )(*[pltpu.with_memory_space_constraint(x, pltpu.HBM) for x in (queries, keys, values, doc_lengths.reshape(1, docs))])


def solution(mesh):
    return jax.shard_map(
        on_device,
        mesh=mesh,
        in_specs=(P(("grp", "cp"), None), P(("grp", "cp"), None), P(("grp", "cp"), None), P("grp")),
        out_specs=P(("grp", "cp"), None),
        check_vma=False,
    )
```

```python
import functools
import math

import jax
import jax.numpy as jnp
from jax import lax
from jax.experimental import pallas as pl
from jax.experimental.pallas import tpu as pltpu
from jax.sharding import PartitionSpec as P

DH = 128
T = 512
B = 128
C = 512
LAG = 3
BIG = 32768.0
NEG = -1e30
SCALE = 144.0 ** (-0.5) * math.log2(math.e)
MESH = pl.DeviceIdType.MESH
F32, BF16, I32 = jnp.float32, jnp.bfloat16, jnp.int32


def stacked(pair):
    return jnp.concatenate([pair[:, :DH], pair[:, DH:]], axis=0)


def kernel(
    q_hbm, k_hbm, v_hbm, len_ref, o_ref,
    kv, qv, qr, raw, msg, held, tops, stat_s, stat_r, augk, augq, augr, flags,
    loc_sem, q_send, q_recv, own_send, own_recv, msg_send, msg_recv,
    st_send, st_recv, fwd_send, fwd_recv,
):
    hk = kv.shape[0]
    n = lax.axis_size("cp")
    me = lax.axis_index("cp")
    core = lax.rem(me, 2)
    chip = lax.div(me, 2)
    partner = me + 1 - 2 * core
    next_head = lax.rem(me + 2 - core, n)
    last_head = lax.rem(me + n - 2, n)
    last_tail = lax.rem(me + n - 1, n)
    own0 = pl.multiple_of(T + T * core, T)
    barrier = pltpu.get_barrier_semaphore()
    half = T // 2

    def lanes(h, width):
        return pl.ds(pl.multiple_of(h * width, DH), width)

    def local(h):
        mine = pl.ds(own0, T)
        return (
            pltpu.make_async_copy(k_hbm.at[:, lanes(h, DH)], kv.at[h, mine, pl.ds(0, DH)], loc_sem.at[0, h]),
            pltpu.make_async_copy(v_hbm.at[:, lanes(h, DH)], raw.at[h], loc_sem.at[1, h]),
            pltpu.make_async_copy(q_hbm.at[:, lanes(h, 2 * DH)], qv.at[h], loc_sem.at[2, h]),
        )

    def remote(src, dst, send, recv, to):
        return pltpu.make_async_remote_copy(src, dst, send, recv, device_id={"cp": to}, device_id_type=MESH)

    def send_q(h, part):
        src = qv.at[h, pl.ds(part * half, half)]
        return remote(src, qr.at[h], q_send.at[part, h], q_recv.at[h], (last_head, last_tail)[part])

    def send_own(h):
        mine = kv.at[h, pl.ds(own0, T)]
        return remote(mine, mine, own_send.at[h], own_recv.at[h], partner)

    def send_msg(h, part):
        dst = kv.at[h, pl.ds(part * half, half)]
        return remote(msg.at[h], dst, msg_send.at[h], msg_recv.at[part, h], next_head)

    def send_stat(h, part):
        return remote(stat_s.at[h], stat_r.at[part, h], st_send.at[h], st_recv.at[part, h], next_head)

    def forward(h):
        part = kv.at[h, pl.ds(0, T)]
        return remote(part, part, fwd_send.at[h], fwd_recv.at[h], partner)

    def every(body):
        def step(h, carry):
            body(h)
            return carry

        lax.fori_loop(0, hk, step, 0)

    def start_local(which):
        def start(h):
            local(h)[which].start()

        return start

    for which in (2, 1, 0):
        every(start_local(which))

    has_left = chip > 0
    has_right = chip < lax.div(n, 2) - 1

    def greet(other):
        pl.semaphore_signal(barrier, inc=1, device_id={"cp": other}, device_id_type=MESH)

    greet(partner)

    @pl.when(has_right)
    def _():
        greet(next_head)

    @pl.when(has_left & (core == 0))
    def _():
        greet(last_head)
        greet(last_tail)

    right, left = jnp.where(has_right, 1, 0), jnp.where(has_left, 1, 0)
    pl.semaphore_wait(barrier, 1 + right + 2 * left * (1 - core))

    def query(h):
        local(h)[2].wait()

        @pl.when(has_left & (core == 0))
        def _():
            send_q(h, 0).start()
            send_q(h, 1).start()

    every(query)

    @pl.when(chip == 0)
    def _():
        def clear(h):
            kv[h, 0:T] = jnp.zeros((T, 2 * DH), BF16)

        every(clear)

    lens = jnp.broadcast_to(len_ref[...], (8, len_ref.shape[1]))
    docs = lens.shape[1]
    upto = lax.broadcasted_iota(I32, (docs, docs), 0) <= lax.broadcasted_iota(I32, (docs, docs), 1)
    upto = jnp.where(upto, 1.0, 0.0).astype(BF16)
    high = lax.shift_right_logical(lens, 5).astype(F32).astype(BF16)
    low = (lens & 31).astype(F32).astype(BF16)
    ends = 32.0 * jnp.dot(high, upto, preferred_element_type=F32) + jnp.dot(low, upto, preferred_element_type=F32)
    ends = ends[0:1].astype(I32)
    ones = jnp.ones((docs, DH), BF16)

    def doc_of(pos):
        past = jnp.where(pos >= ends, 1.0, 0.0).astype(BF16)
        return jnp.dot(past, ones, preferred_element_type=F32)

    def doc_rows(base, rows):
        return doc_of(lax.broadcasted_iota(I32, (rows, docs), 0) + base)

    def doc_at(p):
        return doc_of(jnp.zeros((8, docs), I32) + p)

    def bits(doc):
        lane = lax.broadcasted_iota(I32, doc.shape, 1)
        return (lax.shift_right_logical(doc.astype(I32), lane & 7) & 1).astype(F32), lane

    def key_side(doc, hidden):
        b, lane = bits(doc)
        out = jnp.where(lane < 8, b - 1.0, jnp.where(lane < 16, -b, jnp.where(lane == 16, -hidden, 0.0)))
        return (out * BIG).astype(BF16)

    def query_side(doc):
        b, lane = bits(doc)
        return jnp.where(lane < 8, b, jnp.where(lane < 16, 1.0 - b, jnp.where(lane == 16, 1.0, 0.0))).astype(BF16)

    first = chip * (2 * T)
    inner = jnp.where(chip > 0, 1.0, 0.0)
    far_left = jnp.where(doc_at(first - T - 1) == doc_at(first), 1.0, 0.0) * inner
    far_right = jnp.where(doc_at(first + T - 1) == doc_at(first + 2 * T), 1.0, 0.0)
    flags[0] = far_left
    flags[1] = far_right
    hidden = jnp.maximum(far_left, 1.0 - inner)[0:1]
    for part in range(3):
        doc = doc_rows(first + (part - 1) * T, T)
        augk[part * T : (part + 1) * T] = key_side(doc, hidden if part == 0 else 0.0)
    augq[...] = query_side(doc_rows(me * T, T))
    augr[...] = query_side(doc_rows(first + 2 * T + core * half, half))

    ones_v = jnp.ones((16, 3 * T), BF16)
    column = lax.broadcasted_iota(I32, (B, 2 * B), 1)
    causal = lax.broadcasted_iota(I32, (B, 2 * B), 0) <= (column & (B - 1))

    def chunks(lo, hi):
        return [(i, min(i + C, hi)) for i in range(lo, hi, C)]

    def scores(h, pair, aug, lo, hi, diagonal):
        q = jnp.concatenate([stacked(pair), jnp.concatenate([aug, aug], axis=0)], axis=1)
        found, top = [], None
        for i, j in chunks(lo, hi):
            k = jnp.concatenate([kv[h, i:j, 0:DH], augk[i:j]], axis=1)
            s = lax.dot_general(k, q, (((1,), (1,)), ((), ())), preferred_element_type=F32)
            if diagonal and j == hi:
                last = jnp.where(causal, s[-B:], NEG)
                s = jnp.concatenate([s[:-B], last], axis=0) if j - i > B else last
            high = jnp.max(s, axis=0, keepdims=True)
            top = high if top is None else jnp.maximum(top, high)
            found.append(s)
            yield
        return found, top * SCALE

    def mixed(h, found, top, lo, hi):
        o = None
        for s, (i, j) in zip(found, chunks(lo, hi)):
            p = jnp.exp2(s * SCALE - top).astype(BF16)
            v = jnp.concatenate([kv[h, k : k + B, DH : 2 * DH] for k in range(i, j, B)], axis=1)
            v = jnp.concatenate([v, ones_v[:, : j - i]], axis=0)
            part = jnp.dot(v, p, preferred_element_type=F32)
            o = part if o is None else o + part
            yield
        return o

    def store(h, r, o):
        rows = slice(r * B, (r + 1) * B)
        o_ref[rows, lanes(2 * h, DH)] = jnp.transpose(o[:, :B]).astype(BF16)
        o_ref[rows, lanes(2 * h + 1, DH)] = jnp.transpose(o[:, B:]).astype(BF16)

    def staggered(blocks):
        behind = None
        for block in [*blocks, None]:
            if block is not None:
                for _ in iter(lambda: next(block), "scored"):
                    if behind is not None:
                        next(behind, None)
            if behind is not None:
                for _ in behind:
                    pass
            behind = block

    def border_block(h, i, part):
        rows = slice(i * B, (i + 1) * B)
        r = part * 2 + i
        lo, hi = T + r * B, 3 * T
        s, top = yield from scores(h, qr[h, rows], augr[rows], lo, hi, False)
        yield "scored"
        o = yield from mixed(h, s, top, lo, hi)
        acc, total = o[:DH], o[DH : DH + 1]
        own = kv[h, 2 * T + r * B : 2 * T + (r + 1) * B].astype(F32)
        msg[h, rows] = jnp.where(flags[1][0:1, 0:1] > 0.5, acc / total, own).astype(BF16)
        stat_s[h, i : i + 1] = top + jnp.log2(total)

    def border(h, part):
        send_q(h, part).wait_recv()
        staggered(border_block(h, i, part) for i in range(2))
        send_msg(h, part).start()
        send_stat(h, part).start()

    def near_block(h, r, core):
        rows = slice(r * B, (r + 1) * B)
        lo, hi = T, T + core * T + (r + 1) * B
        s, top = yield from scores(h, qv[h, rows], augq[rows], lo, hi, True)
        yield "scored"
        held[h, r] = yield from mixed(h, s, top, lo, hi)
        tops[h, r : r + 1] = top

    def far_block(h, r, core):
        rows = slice(r * B, (r + 1) * B)
        lo, hi = core * r * B, T
        s, top = yield from scores(h, qv[h, rows], augq[rows], lo, hi, False)
        yield "scored"
        before = tops[h, r : r + 1]
        top = jnp.maximum(top, before)
        if core == 0:
            level = jnp.where(flags[0][0:1, 0:1] > 0.5, stat_r[r // 2, h, r % 2 : r % 2 + 1], NEG)
            top = jnp.maximum(top, level)
        o = yield from mixed(h, s, top, lo, hi)
        o = o + held[h, r] * jnp.exp2(before - top)
        acc, total = o[:DH], o[DH : DH + 1]
        if core == 0:
            weight = jnp.exp2(level - top)
            acc, total = acc + weight * kv[h, rows].astype(F32), total + weight
        store(h, r, acc / total)

    def turn(h):
        for copy in local(h)[:2]:
            copy.wait()
        for i in range(0, T, DH):
            block = jnp.transpose(raw[h, i : i + DH].astype(F32)).astype(BF16)
            kv[h, pl.ds(pl.multiple_of(own0 + i, DH), DH), DH : 2 * DH] = block

    def share(h, carry):
        @pl.when(h < hk)
        def _():
            turn(h)

        @pl.when(h > 0)
        def _():
            send_own(h - 1).start()

        return carry

    lax.fori_loop(0, hk + 1, share, 0)

    @pl.when(core == 0)
    def _():
        def step(it, carry):
            h = it - LAG

            @pl.when((it >= LAG) & has_left)
            def _():
                for part in range(2):
                    send_msg(h, part).wait_recv()
                    send_stat(h, part).wait_recv()
                forward(h).start()

            @pl.when(it < hk)
            def _():
                send_own(it).wait_recv()

                @pl.when(has_right)
                def _():
                    border(it, 0)

                staggered(near_block(it, r, 0) for r in range(T // B))

            @pl.when(it >= LAG)
            def _():
                staggered(far_block(h, r, 0) for r in range(T // B))

            return carry

        lax.fori_loop(0, hk + LAG, step, 0)

        def finish(h):
            send_own(h).wait_send()

            @pl.when(has_left)
            def _():
                for part in range(2):
                    send_q(h, part).wait_send()
                forward(h).wait_send()

            @pl.when(has_right)
            def _():
                send_msg(h, 0).wait_send()
                send_stat(h, 0).wait_send()

        every(finish)

    @pl.when(core == 1)
    def _():
        def step(it, carry):
            h = it - LAG

            @pl.when(it < hk)
            def _():
                send_own(it).wait_recv()

                @pl.when(has_right)
                def _():
                    border(it, 1)

                staggered(near_block(it, r, 1) for r in range(T // B))

            @pl.when(it >= LAG)
            def _():
                @pl.when(has_left)
                def _():
                    forward(h).wait_recv()

                staggered(far_block(h, r, 1) for r in range(T // B))

            return carry

        lax.fori_loop(0, hk + LAG, step, 0)

        def finish(h):
            send_own(h).wait_send()

            @pl.when(has_right)
            def _():
                send_msg(h, 1).wait_send()
                send_stat(h, 1).wait_send()

        every(finish)


def on_device(queries, keys, values, doc_lengths):
    hk = keys.shape[1] // DH
    docs = doc_lengths.shape[0]
    sem = pltpu.SemaphoreType.DMA
    hbm = pl.BlockSpec(memory_space=pltpu.HBM)
    vmem = pl.BlockSpec(memory_space=pltpu.VMEM)
    return pl.pallas_call(
        kernel,
        out_shape=pltpu.VMEM(queries.shape, BF16),
        in_specs=[hbm, hbm, hbm, vmem],
        out_specs=vmem,
        scratch_shapes=[
            pltpu.VMEM((hk, 3 * T, 2 * DH), BF16),
            pltpu.VMEM((hk, T, 2 * DH), BF16),
            pltpu.VMEM((hk, T // 2, 2 * DH), BF16),
            pltpu.VMEM((hk, T, DH), BF16),
            pltpu.VMEM((hk, T // 2, 2 * DH), BF16),
            pltpu.VMEM((hk, T // B, DH + 16, 2 * B), F32),
            pltpu.VMEM((hk, 8, 2 * B), F32),
            pltpu.VMEM((hk, 8, 2 * B), F32),
            pltpu.VMEM((2, hk, 8, 2 * B), F32),
            pltpu.VMEM((3 * T, DH), BF16),
            pltpu.VMEM((T, DH), BF16),
            pltpu.VMEM((T // 2, DH), BF16),
            pltpu.VMEM((2, 8, DH), F32),
            sem((3, hk)),
            sem((2, hk)),
            sem((hk,)),
            sem((hk,)),
            sem((hk,)),
            sem((hk,)),
            sem((2, hk)),
            sem((hk,)),
            sem((2, hk)),
            sem((hk,)),
            sem((hk,)),
        ],
        compiler_params=pltpu.CompilerParams(
            collective_id=0, has_side_effects=True, vmem_limit_bytes=36 * 1024 * 1024
        ),
    )(*[pltpu.with_memory_space_constraint(x, pltpu.HBM) for x in (queries, keys, values, doc_lengths.reshape(1, docs))])


def solution(mesh):
    return jax.shard_map(
        on_device,
        mesh=mesh,
        in_specs=(P(("grp", "cp"), None), P(("grp", "cp"), None), P(("grp", "cp"), None), P("grp")),
        out_specs=P(("grp", "cp"), None),
        check_vma=False,
    )
```

```python
import functools
import math

import jax
import jax.numpy as jnp
from jax import lax
from jax.experimental import pallas as pl
from jax.experimental.pallas import tpu as pltpu
from jax.sharding import PartitionSpec as P

DH = 128
T = 512
B = 128
C = 512
LAG = 3
FIRST_LAG, LAST_LAG = 5, 6
LINE = 8
BIG = 32768.0
NEG = -1e30
SCALE = 144.0 ** (-0.5) * math.log2(math.e)
MESH = pl.DeviceIdType.MESH
F32, BF16, I32 = jnp.float32, jnp.bfloat16, jnp.int32


def stacked(pair):
    return jnp.concatenate([pair[:, :DH], pair[:, DH:]], axis=0)


def kernel(
    q_hbm, k_hbm, v_hbm, len_ref, o_ref,
    kv, qv, qr, raw, msg, held, tops, stat_s, stat_r, early, augk, augq, augr, flags,
    loc_sem, q_send, q_recv, own_send, own_recv, msg_send, msg_recv,
    st_send, st_recv, fwd_send, fwd_recv, whole_send, whole_recv,
):
    hk = kv.shape[0]
    n = lax.axis_size("cp")
    me = lax.axis_index("cp")
    core = lax.rem(me, 2)
    chip = lax.div(me, 2)
    partner = me + 1 - 2 * core
    next_head = lax.rem(me + 2 - core, n)
    last_head = lax.rem(me + n - 2, n)
    last_tail = lax.rem(me + n - 1, n)
    own0 = pl.multiple_of(T + T * core, T)
    barrier = pltpu.get_barrier_semaphore()
    half = T // 2

    def lanes(h, width):
        return pl.ds(pl.multiple_of(h * width, DH), width)

    def local(h):
        mine = pl.ds(own0, T)
        return (
            pltpu.make_async_copy(k_hbm.at[:, lanes(h, DH)], kv.at[h, mine, pl.ds(0, DH)], loc_sem.at[0, h]),
            pltpu.make_async_copy(v_hbm.at[:, lanes(h, DH)], raw.at[h], loc_sem.at[1, h]),
            pltpu.make_async_copy(q_hbm.at[:, lanes(h, 2 * DH)], qv.at[h], loc_sem.at[2, h]),
        )

    def remote(src, dst, send, recv, to):
        return pltpu.make_async_remote_copy(src, dst, send, recv, device_id={"cp": to}, device_id_type=MESH)

    def send_q(h, part):
        src = qv.at[h, pl.ds(part * half, half)]
        return remote(src, qr.at[h], q_send.at[part, h], q_recv.at[h], (last_head, last_tail)[part])

    def send_own(h):
        mine = kv.at[h, pl.ds(own0, T)]
        return remote(mine, mine, own_send.at[h], own_recv.at[h], partner)

    def send_msg(h, part):
        dst = kv.at[h, pl.ds(part * half, half)]
        return remote(msg.at[h], dst, msg_send.at[h], msg_recv.at[part, h], next_head)

    def send_stat(h, part):
        return remote(stat_s.at[h], stat_r.at[part, h], st_send.at[h], st_recv.at[part, h], next_head)

    def send_whole(part):
        src = kv.at[hk - 1, pl.ds(T + part * T, T)]
        dst = (early, kv.at[hk - 1, pl.ds(0, T)])[part]
        return remote(src, dst, whole_send, (whole_recv, msg_recv.at[0, hk - 1])[part], next_head)

    def forward(h):
        part = kv.at[h, pl.ds(0, T)]
        return remote(part, part, fwd_send.at[h], fwd_recv.at[h], partner)

    def every(body):
        def step(h, carry):
            body(h)
            return carry

        lax.fori_loop(0, hk, step, 0)

    def start_local(which):
        def start(h):
            local(h)[which].start()

        return start

    for which in (2, 1, 0):
        every(start_local(which))

    place = lax.rem(chip, LINE)
    lag = jnp.where(place == 0, FIRST_LAG, jnp.where(place == LINE - 1, LAST_LAG, LAG))
    has_left = chip > 0
    has_right = chip < lax.div(n, 2) - 1

    def greet(other):
        pl.semaphore_signal(barrier, inc=1, device_id={"cp": other}, device_id_type=MESH)

    greet(partner)

    @pl.when(has_right)
    def _():
        greet(next_head)

    @pl.when(has_left & (core == 0))
    def _():
        greet(last_head)
        greet(last_tail)

    right, left = jnp.where(has_right, 1, 0), jnp.where(has_left, 1, 0)
    pl.semaphore_wait(barrier, 1 + right + 2 * left * (1 - core))

    def query(h):
        local(h)[2].wait()

        @pl.when(has_left & (core == 0))
        def _():
            @pl.when(h < hk - 1)
            def _():
                send_q(h, 0).start()
                send_q(h, 1).start()

    every(query)

    @pl.when(chip == 0)
    def _():
        def clear(h):
            kv[h, 0:T] = jnp.zeros((T, 2 * DH), BF16)

        every(clear)
        early[...] = jnp.zeros((T, 2 * DH), BF16)

    def turn(h):
        for copy in local(h)[:2]:
            copy.wait()
        for i in range(0, T, DH):
            block = jnp.transpose(raw[h, i : i + DH].astype(F32)).astype(BF16)
            kv[h, pl.ds(pl.multiple_of(own0 + i, DH), DH), DH : 2 * DH] = block

    def share(i, carry):
        @pl.when(i < hk)
        def _():
            turn(lax.rem(i + hk - 1, hk))

        @pl.when(i > 0)
        def _():
            send_own(lax.rem(i + hk - 2, hk)).start()

        @pl.when((i == 1) & has_right)
        def _():
            @pl.when(core == 0)
            def _():
                send_whole(0).start()

            @pl.when(core == 1)
            def _():
                send_whole(1).start()

        return carry

    lax.fori_loop(0, hk + 1, share, 0)

    lens = jnp.broadcast_to(len_ref[...], (8, len_ref.shape[1]))
    docs = lens.shape[1]
    upto = lax.broadcasted_iota(I32, (docs, docs), 0) <= lax.broadcasted_iota(I32, (docs, docs), 1)
    upto = jnp.where(upto, 1.0, 0.0).astype(BF16)
    high = lax.shift_right_logical(lens, 5).astype(F32).astype(BF16)
    low = (lens & 31).astype(F32).astype(BF16)
    ends = 32.0 * jnp.dot(high, upto, preferred_element_type=F32) + jnp.dot(low, upto, preferred_element_type=F32)
    ends = ends[0:1].astype(I32)
    ones = jnp.ones((docs, DH), BF16)

    def doc_of(pos):
        past = jnp.where(pos >= ends, 1.0, 0.0).astype(BF16)
        return jnp.dot(past, ones, preferred_element_type=F32)

    def doc_rows(base, rows):
        return doc_of(lax.broadcasted_iota(I32, (rows, docs), 0) + base)

    def doc_at(p):
        return doc_of(jnp.zeros((8, docs), I32) + p)

    def bits(doc):
        lane = lax.broadcasted_iota(I32, doc.shape, 1)
        return (lax.shift_right_logical(doc.astype(I32), lane & 7) & 1).astype(F32), lane

    def key_side(doc, hidden):
        b, lane = bits(doc)
        out = jnp.where(lane < 8, b - 1.0, jnp.where(lane < 16, -b, jnp.where(lane == 16, -hidden, 0.0)))
        return (out * BIG).astype(BF16)

    def query_side(doc):
        b, lane = bits(doc)
        return jnp.where(lane < 8, b, jnp.where(lane < 16, 1.0 - b, jnp.where(lane == 16, 1.0, 0.0))).astype(BF16)

    first = chip * (2 * T)
    inner = jnp.where(chip > 0, 1.0, 0.0)
    far_left = jnp.where(doc_at(first - T - 1) == doc_at(first), 1.0, 0.0) * inner
    far_right = jnp.where(doc_at(first + T - 1) == doc_at(first + 2 * T), 1.0, 0.0)
    flags[0] = far_left
    flags[1] = far_right
    hidden = jnp.maximum(far_left, 1.0 - inner)[0:1]
    for part in range(3):
        doc = doc_rows(first + (part - 1) * T, T)
        augk[part * T : (part + 1) * T] = key_side(doc, hidden if part == 0 else 0.0)
        if part == 0:
            augk[4 * T : 5 * T] = key_side(doc, 1.0 - inner)
    augk[3 * T : 4 * T] = key_side(doc_rows(first - 2 * T, T), 1.0 - inner)
    augq[...] = query_side(doc_rows(me * T, T))
    augr[...] = query_side(doc_rows(first + 2 * T + core * half, half))

    ones_v = jnp.ones((16, 3 * T), BF16)
    column = lax.broadcasted_iota(I32, (B, 2 * B), 1)
    causal = lax.broadcasted_iota(I32, (B, 2 * B), 0) <= (column & (B - 1))

    def chunks(lo, hi):
        if lo < 0 < hi:
            return chunks(lo, 0) + chunks(0, hi)
        return [(i, min(i + C, hi)) for i in range(lo, hi, C)]

    def rows_of(h, i, j):
        return early[i + T : j + T] if i < 0 else kv[h, i:j]

    def aug_of(i, j, last):
        return augk[i + 4 * T : j + 4 * T] if last and j <= T else augk[i:j]

    def scores(h, pair, aug, lo, hi, diagonal, last=False):
        q = jnp.concatenate([stacked(pair), jnp.concatenate([aug, aug], axis=0)], axis=1)
        found, top = [], None
        for i, j in chunks(lo, hi):
            k = jnp.concatenate([rows_of(h, i, j)[:, 0:DH], aug_of(i, j, last)], axis=1)
            s = lax.dot_general(k, q, (((1,), (1,)), ((), ())), preferred_element_type=F32)
            if diagonal and j == hi:
                end = jnp.where(causal, s[-B:], NEG)
                s = jnp.concatenate([s[:-B], end], axis=0) if j - i > B else end
            high = jnp.max(s, axis=0, keepdims=True)
            top = high if top is None else jnp.maximum(top, high)
            found.append(s)
            yield
        return found, top * SCALE

    def mixed(h, found, top, lo, hi):
        o = None
        for s, (i, j) in zip(found, chunks(lo, hi)):
            p = jnp.exp2(s * SCALE - top).astype(BF16)
            v = jnp.concatenate([rows_of(h, k, k + B)[:, DH : 2 * DH] for k in range(i, j, B)], axis=1)
            v = jnp.concatenate([v, ones_v[:, : j - i]], axis=0)
            part = jnp.dot(v, p, preferred_element_type=F32)
            o = part if o is None else o + part
            yield
        return o

    def store(h, r, o):
        rows = slice(r * B, (r + 1) * B)
        o_ref[rows, lanes(2 * h, DH)] = jnp.transpose(o[:, :B]).astype(BF16)
        o_ref[rows, lanes(2 * h + 1, DH)] = jnp.transpose(o[:, B:]).astype(BF16)

    def staggered(blocks):
        behind = None
        for block in [*blocks, None]:
            if block is not None:
                for _ in iter(lambda: next(block), "scored"):
                    if behind is not None:
                        next(behind, None)
            if behind is not None:
                for _ in behind:
                    pass
            behind = block

    def border_block(h, i, part):
        rows = slice(i * B, (i + 1) * B)
        r = part * 2 + i
        lo, hi = T + r * B, 3 * T
        s, top = yield from scores(h, qr[h, rows], augr[rows], lo, hi, False)
        yield "scored"
        o = yield from mixed(h, s, top, lo, hi)
        acc, total = o[:DH], o[DH : DH + 1]
        own = kv[h, 2 * T + r * B : 2 * T + (r + 1) * B].astype(F32)
        msg[h, rows] = jnp.where(flags[1][0:1, 0:1] > 0.5, acc / total, own).astype(BF16)
        stat_s[h, i : i + 1] = top + jnp.log2(total)

    def border(h, part):
        send_q(h, part).wait_recv()
        staggered(border_block(h, i, part) for i in range(2))
        send_msg(h, part).start()
        send_stat(h, part).start()

    def near_block(h, r, core):
        rows = slice(r * B, (r + 1) * B)
        lo, hi = T, T + core * T + (r + 1) * B
        s, top = yield from scores(h, qv[h, rows], augq[rows], lo, hi, True)
        yield "scored"
        held[h, r] = yield from mixed(h, s, top, lo, hi)
        tops[h, r : r + 1] = top

    def far_block(h, r, core, last=False):
        rows = slice(r * B, (r + 1) * B)
        lo, hi = core * r * B, T
        if last and core == 0:
            lo = r * B - T
        s, top = yield from scores(h, qv[h, rows], augq[rows], lo, hi, False, last)
        yield "scored"
        before = tops[h, r : r + 1]
        top = jnp.maximum(top, before)
        if core == 0 and not last:
            level = jnp.where(flags[0][0:1, 0:1] > 0.5, stat_r[r // 2, h, r % 2 : r % 2 + 1], NEG)
            top = jnp.maximum(top, level)
        o = yield from mixed(h, s, top, lo, hi)
        o = o + held[h, r] * jnp.exp2(before - top)
        acc, total = o[:DH], o[DH : DH + 1]
        if core == 0 and not last:
            weight = jnp.exp2(level - top)
            acc, total = acc + weight * kv[h, rows].astype(F32), total + weight
        store(h, r, acc / total)

    @pl.when(core == 0)
    def _():
        def step(it, carry):
            h = it - lag

            @pl.when((it >= lag) & (h < hk - 1) & has_left)
            def _():
                for part in range(2):
                    send_msg(h, part).wait_recv()
                    send_stat(h, part).wait_recv()
                forward(h).start()

            @pl.when((it == min(4, hk - 1)) & has_left)
            def _():
                send_whole(1).wait_recv()
                forward(hk - 1).start()

            @pl.when(it < hk)
            def _():
                send_own(it).wait_recv()

                @pl.when(has_right & (it < hk - 1))
                def _():
                    border(it, 0)

                staggered(near_block(it, r, 0) for r in range(T // B))

            @pl.when((it >= lag) & (h < hk - 1))
            def _():
                staggered(far_block(h, r, 0) for r in range(T // B))

            @pl.when(it == hk - 1)
            def _():
                @pl.when(has_left)
                def _():
                    send_whole(0).wait_recv()

                staggered(far_block(hk - 1, r, 0, True) for r in range(T // B))

            return carry

        lax.fori_loop(0, hk + LAST_LAG - 1, step, 0)

        def finish(h):
            send_own(h).wait_send()

            @pl.when(has_left)
            def _():
                forward(h).wait_send()

            @pl.when(has_left & (h < hk - 1))
            def _():
                for part in range(2):
                    send_q(h, part).wait_send()

            @pl.when(has_right & (h < hk - 1))
            def _():
                send_msg(h, 0).wait_send()
                send_stat(h, 0).wait_send()

            @pl.when(has_right & (h == hk - 1))
            def _():
                send_whole(0).wait_send()

        every(finish)

    @pl.when(core == 1)
    def _():
        def step(it, carry):
            h = it - lag

            @pl.when(it < hk)
            def _():
                send_own(it).wait_recv()

                @pl.when(has_right & (it < hk - 1))
                def _():
                    border(it, 1)

                staggered(near_block(it, r, 1) for r in range(T // B))

            @pl.when((it >= lag) & (h < hk - 1))
            def _():
                @pl.when(has_left)
                def _():
                    forward(h).wait_recv()

                staggered(far_block(h, r, 1) for r in range(T // B))

            @pl.when(it == hk - 1)
            def _():
                @pl.when(has_left)
                def _():
                    forward(hk - 1).wait_recv()

                staggered(far_block(hk - 1, r, 1, True) for r in range(T // B))

            return carry

        lax.fori_loop(0, hk + LAST_LAG - 1, step, 0)

        def finish(h):
            send_own(h).wait_send()

            @pl.when(has_right & (h < hk - 1))
            def _():
                send_msg(h, 1).wait_send()
                send_stat(h, 1).wait_send()

            @pl.when(has_right & (h == hk - 1))
            def _():
                send_whole(1).wait_send()

        every(finish)


def on_device(queries, keys, values, doc_lengths):
    hk = keys.shape[1] // DH
    docs = doc_lengths.shape[0]
    sem = pltpu.SemaphoreType.DMA
    hbm = pl.BlockSpec(memory_space=pltpu.HBM)
    vmem = pl.BlockSpec(memory_space=pltpu.VMEM)
    return pl.pallas_call(
        kernel,
        out_shape=pltpu.VMEM(queries.shape, BF16),
        in_specs=[hbm, hbm, hbm, vmem],
        out_specs=vmem,
        scratch_shapes=[
            pltpu.VMEM((hk, 3 * T, 2 * DH), BF16),
            pltpu.VMEM((hk, T, 2 * DH), BF16),
            pltpu.VMEM((hk, T // 2, 2 * DH), BF16),
            pltpu.VMEM((hk, T, DH), BF16),
            pltpu.VMEM((hk, T // 2, 2 * DH), BF16),
            pltpu.VMEM((hk, T // B, DH + 16, 2 * B), F32),
            pltpu.VMEM((hk, 8, 2 * B), F32),
            pltpu.VMEM((hk, 8, 2 * B), F32),
            pltpu.VMEM((2, hk, 8, 2 * B), F32),
            pltpu.VMEM((T, 2 * DH), BF16),
            pltpu.VMEM((5 * T, DH), BF16),
            pltpu.VMEM((T, DH), BF16),
            pltpu.VMEM((T // 2, DH), BF16),
            pltpu.VMEM((2, 8, DH), F32),
            sem((3, hk)),
            sem((2, hk)),
            sem((hk,)),
            sem((hk,)),
            sem((hk,)),
            sem((hk,)),
            sem((2, hk)),
            sem((hk,)),
            sem((2, hk)),
            sem((hk,)),
            sem((hk,)),
            sem,
            sem,
        ],
        compiler_params=pltpu.CompilerParams(
            collective_id=0, has_side_effects=True, vmem_limit_bytes=36 * 1024 * 1024
        ),
    )(*[pltpu.with_memory_space_constraint(x, pltpu.HBM) for x in (queries, keys, values, doc_lengths.reshape(1, docs))])


def solution(mesh):
    return jax.shard_map(
        on_device,
        mesh=mesh,
        in_specs=(P(("grp", "cp"), None), P(("grp", "cp"), None), P(("grp", "cp"), None), P("grp")),
        out_specs=P(("grp", "cp"), None),
        check_vma=False,
    )
```

```python
import functools
import math

import jax
import jax.numpy as jnp
from jax import lax
from jax.experimental import pallas as pl
from jax.experimental.pallas import tpu as pltpu
from jax.sharding import PartitionSpec as P

DH = 128
T = 512
B = 128
BORDER, NEAR, FAR, WHOLE = 512, (256, 512), 256, 512
LAG = 3
FIRST_LAG, LAST_LAG = 4, 5
LINE = 8
BIG = 32768.0
NEG = -1e30
SCALE = 144.0 ** (-0.5) * math.log2(math.e)
MESH = pl.DeviceIdType.MESH
F32, BF16, I32 = jnp.float32, jnp.bfloat16, jnp.int32


def stacked(pair):
    return jnp.concatenate([pair[:, :DH], pair[:, DH:]], axis=0)


def kernel(
    q_hbm, k_hbm, v_hbm, len_hbm, o_ref,
    kv, qv, qr, raw, msg, held, tops, stat_s, stat_r, early, augk, augq, augr, flags, len_ref,
    loc_sem, q_send, q_recv, own_send, own_recv, msg_send, msg_recv,
    st_send, st_recv, fwd_send, fwd_recv, whole_send, whole_recv, len_sem,
):
    hk = kv.shape[0]
    n = lax.axis_size("cp")
    me = lax.axis_index("cp")
    core = lax.rem(me, 2)
    chip = lax.div(me, 2)
    partner = me + 1 - 2 * core
    next_head = lax.rem(me + 2 - core, n)
    last_head = lax.rem(me + n - 2, n)
    last_tail = lax.rem(me + n - 1, n)
    own0 = pl.multiple_of(T + T * core, T)
    barrier = pltpu.get_barrier_semaphore()
    half = T // 2

    def lanes(h, width):
        return pl.ds(pl.multiple_of(h * width, DH), width)

    def local(h):
        mine = pl.ds(own0, T)
        return (
            pltpu.make_async_copy(k_hbm.at[:, lanes(h, DH)], kv.at[h, mine, pl.ds(0, DH)], loc_sem.at[0, h]),
            pltpu.make_async_copy(v_hbm.at[:, lanes(h, DH)], raw.at[h], loc_sem.at[1, h]),
            pltpu.make_async_copy(q_hbm.at[:, lanes(h, 2 * DH)], qv.at[h], loc_sem.at[2, h]),
        )

    def remote(src, dst, send, recv, to):
        return pltpu.make_async_remote_copy(src, dst, send, recv, device_id={"cp": to}, device_id_type=MESH)

    def send_q(h, part):
        src = qv.at[h, pl.ds(part * half, half)]
        return remote(src, qr.at[h], q_send.at[part, h], q_recv.at[h], (last_head, last_tail)[part])

    def send_own(h):
        mine = kv.at[h, pl.ds(own0, T)]
        return remote(mine, mine, own_send.at[h], own_recv.at[h], partner)

    def send_msg(h, part):
        dst = kv.at[h, pl.ds(part * half, half)]
        return remote(msg.at[h], dst, msg_send.at[h], msg_recv.at[part, h], next_head)

    def send_stat(h, part):
        return remote(stat_s.at[h], stat_r.at[part, h], st_send.at[h], st_recv.at[part, h], next_head)

    def send_whole(part):
        src = kv.at[hk - 1, pl.ds(T + part * T, T)]
        dst = (early, kv.at[hk - 1, pl.ds(0, T)])[part]
        return remote(src, dst, whole_send, (whole_recv, msg_recv.at[0, hk - 1])[part], next_head)

    def forward(h):
        part = kv.at[h, pl.ds(0, T)]
        return remote(part, part, fwd_send.at[h], fwd_recv.at[h], partner)

    def every(body):
        def step(h, carry):
            body(h)
            return carry

        lax.fori_loop(0, hk, step, 0)

    def start_local(which):
        def start(h):
            local(h)[which].start()

        return start

    lengths = pltpu.make_async_copy(len_hbm, len_ref, len_sem)
    lengths.start()
    for which in (2, 1, 0):
        every(start_local(which))

    place = lax.rem(chip, LINE)
    lag = jnp.where(place == 0, FIRST_LAG, jnp.where(place == LINE - 1, LAST_LAG, LAG))
    has_left = chip > 0
    has_right = chip < lax.div(n, 2) - 1

    def greet(other):
        pl.semaphore_signal(barrier, inc=1, device_id={"cp": other}, device_id_type=MESH)

    greet(partner)

    @pl.when(has_right)
    def _():
        greet(next_head)

    @pl.when(has_left & (core == 0))
    def _():
        greet(last_head)
        greet(last_tail)

    right, left = jnp.where(has_right, 1, 0), jnp.where(has_left, 1, 0)
    pl.semaphore_wait(barrier, 1 + right + 2 * left * (1 - core))

    def query(h):
        local(h)[2].wait()

        @pl.when(has_left & (core == 0))
        def _():
            @pl.when(h < hk - 1)
            def _():
                send_q(h, 0).start()
                send_q(h, 1).start()

    every(query)

    @pl.when(chip == 0)
    def _():
        def clear(h):
            kv[h, 0:T] = jnp.zeros((T, 2 * DH), BF16)

        every(clear)
        early[...] = jnp.zeros((T, 2 * DH), BF16)

    def turn(h):
        for copy in local(h)[:2]:
            copy.wait()
        for i in range(0, T, DH):
            block = jnp.transpose(raw[h, i : i + DH].astype(F32)).astype(BF16)
            kv[h, pl.ds(pl.multiple_of(own0 + i, DH), DH), DH : 2 * DH] = block

    def share(i, carry):
        @pl.when(i < hk)
        def _():
            turn(lax.rem(i + hk - 1, hk))

        @pl.when(i > 0)
        def _():
            send_own(lax.rem(i + hk - 2, hk)).start()

        @pl.when((i == 1) & has_right)
        def _():
            @pl.when(core == 0)
            def _():
                send_whole(0).start()

            @pl.when(core == 1)
            def _():
                send_whole(1).start()

        return carry

    lax.fori_loop(0, hk + 1, share, 0)

    lengths.wait()
    lens = jnp.broadcast_to(len_ref[...], (8, len_ref.shape[1]))
    docs = lens.shape[1]
    upto = lax.broadcasted_iota(I32, (docs, docs), 0) <= lax.broadcasted_iota(I32, (docs, docs), 1)
    upto = jnp.where(upto, 1.0, 0.0).astype(BF16)
    high = lax.shift_right_logical(lens, 5).astype(F32).astype(BF16)
    low = (lens & 31).astype(F32).astype(BF16)
    ends = 32.0 * jnp.dot(high, upto, preferred_element_type=F32) + jnp.dot(low, upto, preferred_element_type=F32)
    ends = ends[0:1].astype(I32)
    ones = jnp.ones((docs, DH), BF16)

    def doc_of(pos):
        past = jnp.where(pos >= ends, 1.0, 0.0).astype(BF16)
        return jnp.dot(past, ones, preferred_element_type=F32)

    def doc_rows(base, rows):
        return doc_of(lax.broadcasted_iota(I32, (rows, docs), 0) + base)

    def doc_at(p):
        return doc_of(jnp.zeros((8, docs), I32) + p)

    def bits(doc):
        lane = lax.broadcasted_iota(I32, doc.shape, 1)
        return (lax.shift_right_logical(doc.astype(I32), lane & 7) & 1).astype(F32), lane

    def key_side(doc, hidden):
        b, lane = bits(doc)
        out = jnp.where(lane < 8, b - 1.0, jnp.where(lane < 16, -b, jnp.where(lane == 16, -hidden, 0.0)))
        return (out * BIG).astype(BF16)

    def query_side(doc):
        b, lane = bits(doc)
        return jnp.where(lane < 8, b, jnp.where(lane < 16, 1.0 - b, jnp.where(lane == 16, 1.0, 0.0))).astype(BF16)

    first = chip * (2 * T)
    inner = jnp.where(chip > 0, 1.0, 0.0)
    far_left = jnp.where(doc_at(first - T - 1) == doc_at(first), 1.0, 0.0) * inner
    far_right = jnp.where(doc_at(first + T - 1) == doc_at(first + 2 * T), 1.0, 0.0)
    flags[0] = far_left
    flags[1] = far_right
    hidden = jnp.maximum(far_left, 1.0 - inner)[0:1]
    for part in range(3):
        doc = doc_rows(first + (part - 1) * T, T)
        augk[part * T : (part + 1) * T] = key_side(doc, hidden if part == 0 else 0.0)
        if part == 0:
            augk[4 * T : 5 * T] = key_side(doc, 1.0 - inner)
    augk[3 * T : 4 * T] = key_side(doc_rows(first - 2 * T, T), 1.0 - inner)
    augq[...] = query_side(doc_rows(me * T, T))
    augr[...] = query_side(doc_rows(first + 2 * T + core * half, half))

    ones_v = jnp.ones((16, 3 * T), BF16)
    column = lax.broadcasted_iota(I32, (B, 2 * B), 1)
    causal = lax.broadcasted_iota(I32, (B, 2 * B), 0) <= (column & (B - 1))

    def chunks(lo, hi, size):
        if lo < 0 < hi:
            return chunks(lo, 0, size) + chunks(0, hi, size)
        return [(i, min(i + size, hi)) for i in range(lo, hi, size)]

    def rows_of(h, i, j):
        return early[i + T : j + T] if i < 0 else kv[h, i:j]

    def aug_of(i, j, last):
        return augk[i + 4 * T : j + 4 * T] if last and j <= T else augk[i:j]

    def scores(h, pair, aug, lo, hi, size, diagonal, last=False):
        q = jnp.concatenate([stacked(pair), jnp.concatenate([aug, aug], axis=0)], axis=1)
        found, top = [], None
        for i, j in chunks(lo, hi, size):
            k = jnp.concatenate([rows_of(h, i, j)[:, 0:DH], aug_of(i, j, last)], axis=1)
            s = lax.dot_general(k, q, (((1,), (1,)), ((), ())), preferred_element_type=F32)
            if diagonal and j == hi:
                end = jnp.where(causal, s[-B:], NEG)
                s = jnp.concatenate([s[:-B], end], axis=0) if j - i > B else end
            high = jnp.max(s, axis=0, keepdims=True)
            top = high if top is None else jnp.maximum(top, high)
            found.append(s)
            yield
        return found, top * SCALE

    def mixed(h, found, top, lo, hi, size):
        o = None
        for s, (i, j) in zip(found, chunks(lo, hi, size)):
            p = jnp.exp2(s * SCALE - top).astype(BF16)
            v = jnp.concatenate([rows_of(h, k, k + B)[:, DH : 2 * DH] for k in range(i, j, B)], axis=1)
            v = jnp.concatenate([v, ones_v[:, : j - i]], axis=0)
            part = jnp.dot(v, p, preferred_element_type=F32)
            o = part if o is None else o + part
            yield
        return o

    def store(h, r, o):
        rows = slice(r * B, (r + 1) * B)
        o_ref[rows, lanes(2 * h, DH)] = jnp.transpose(o[:, :B]).astype(BF16)
        o_ref[rows, lanes(2 * h + 1, DH)] = jnp.transpose(o[:, B:]).astype(BF16)

    def staggered(blocks):
        behind = []
        for block in [*blocks, None, None]:
            if block is not None:
                for _ in iter(lambda: next(block), "scored"):
                    if len(behind) > 1:
                        next(behind[0], None)
            if len(behind) > 1 or (block is None and behind):
                for _ in behind.pop(0):
                    pass
            if block is not None:
                behind.append(block)

    def border_block(h, i, part):
        rows = slice(i * B, (i + 1) * B)
        r = part * 2 + i
        lo, hi = T + r * B, 3 * T
        s, top = yield from scores(h, qr[h, rows], augr[rows], lo, hi, BORDER, False)
        yield "scored"
        o = yield from mixed(h, s, top, lo, hi, BORDER)
        acc, total = o[:DH], o[DH : DH + 1]
        own = kv[h, 2 * T + r * B : 2 * T + (r + 1) * B].astype(F32)
        msg[h, rows] = jnp.where(flags[1][0:1, 0:1] > 0.5, acc / total, own).astype(BF16)
        stat_s[h, i : i + 1] = top + jnp.log2(total)

    def border(h, part):
        send_q(h, part).wait_recv()
        staggered(border_block(h, i, part) for i in range(2))
        send_msg(h, part).start()
        send_stat(h, part).start()

    def near_block(h, r, core):
        rows = slice(r * B, (r + 1) * B)
        lo, hi = T, T + core * T + (r + 1) * B
        s, top = yield from scores(h, qv[h, rows], augq[rows], lo, hi, NEAR[core], True)
        yield "scored"
        held[h, r] = yield from mixed(h, s, top, lo, hi, NEAR[core])
        tops[h, r : r + 1] = top

    def far_block(h, r, core, last=False):
        rows = slice(r * B, (r + 1) * B)
        lo, hi, size = core * r * B, T, WHOLE if last else FAR
        if last and core == 0:
            lo = r * B - T
        s, top = yield from scores(h, qv[h, rows], augq[rows], lo, hi, size, False, last)
        yield "scored"
        before = tops[h, r : r + 1]
        top = jnp.maximum(top, before)
        if core == 0 and not last:
            level = jnp.where(flags[0][0:1, 0:1] > 0.5, stat_r[r // 2, h, r % 2 : r % 2 + 1], NEG)
            top = jnp.maximum(top, level)
        o = yield from mixed(h, s, top, lo, hi, size)
        o = o + held[h, r] * jnp.exp2(before - top)
        acc, total = o[:DH], o[DH : DH + 1]
        if core == 0 and not last:
            weight = jnp.exp2(level - top)
            acc, total = acc + weight * kv[h, rows].astype(F32), total + weight
        store(h, r, acc / total)

    @pl.when(core == 0)
    def _():
        def step(it, carry):
            h = it - lag

            @pl.when((it >= lag) & (h < hk - 1) & has_left)
            def _():
                for part in range(2):
                    send_msg(h, part).wait_recv()
                    send_stat(h, part).wait_recv()
                forward(h).start()

            @pl.when((it == min(4, hk - 1)) & has_left)
            def _():
                send_whole(1).wait_recv()
                forward(hk - 1).start()

            @pl.when(it < hk)
            def _():
                send_own(it).wait_recv()

                @pl.when(has_right & (it < hk - 1))
                def _():
                    border(it, 0)

                staggered(near_block(it, r, 0) for r in reversed(range(T // B)))

            @pl.when((it >= lag) & (h < hk - 1))
            def _():
                staggered(far_block(h, r, 0) for r in range(T // B))

            @pl.when(it == hk - 1)
            def _():
                @pl.when(has_left)
                def _():
                    send_whole(0).wait_recv()

                staggered(far_block(hk - 1, r, 0, True) for r in range(T // B))

            return carry

        lax.fori_loop(0, hk + max(FIRST_LAG, LAST_LAG) - 1, step, 0)

        def finish(h):
            send_own(h).wait_send()

            @pl.when(has_left)
            def _():
                forward(h).wait_send()

            @pl.when(has_left & (h < hk - 1))
            def _():
                for part in range(2):
                    send_q(h, part).wait_send()

            @pl.when(has_right & (h < hk - 1))
            def _():
                send_msg(h, 0).wait_send()
                send_stat(h, 0).wait_send()

            @pl.when(has_right & (h == hk - 1))
            def _():
                send_whole(0).wait_send()

        every(finish)

    @pl.when(core == 1)
    def _():
        def step(it, carry):
            h = it - lag

            @pl.when(it < hk)
            def _():
                send_own(it).wait_recv()

                @pl.when(has_right & (it < hk - 1))
                def _():
                    border(it, 1)

                staggered(near_block(it, r, 1) for r in reversed(range(T // B)))

            @pl.when((it >= lag) & (h < hk - 1))
            def _():
                @pl.when(has_left)
                def _():
                    forward(h).wait_recv()

                staggered(far_block(h, r, 1) for r in range(T // B))

            @pl.when(it == hk - 1)
            def _():
                @pl.when(has_left)
                def _():
                    forward(hk - 1).wait_recv()

                staggered(far_block(hk - 1, r, 1, True) for r in range(T // B))

            return carry

        lax.fori_loop(0, hk + max(FIRST_LAG, LAST_LAG) - 1, step, 0)

        def finish(h):
            send_own(h).wait_send()

            @pl.when(has_right & (h < hk - 1))
            def _():
                send_msg(h, 1).wait_send()
                send_stat(h, 1).wait_send()

            @pl.when(has_right & (h == hk - 1))
            def _():
                send_whole(1).wait_send()

        every(finish)


def on_device(queries, keys, values, doc_lengths):
    hk = keys.shape[1] // DH
    docs = doc_lengths.shape[0]
    sem = pltpu.SemaphoreType.DMA
    hbm = pl.BlockSpec(memory_space=pltpu.HBM)
    vmem = pl.BlockSpec(memory_space=pltpu.VMEM)
    return pl.pallas_call(
        kernel,
        out_shape=pltpu.VMEM(queries.shape, BF16),
        in_specs=[hbm, hbm, hbm, hbm],
        out_specs=vmem,
        scratch_shapes=[
            pltpu.VMEM((hk, 3 * T, 2 * DH), BF16),
            pltpu.VMEM((hk, T, 2 * DH), BF16),
            pltpu.VMEM((hk, T // 2, 2 * DH), BF16),
            pltpu.VMEM((hk, T, DH), BF16),
            pltpu.VMEM((hk, T // 2, 2 * DH), BF16),
            pltpu.VMEM((hk, T // B, DH + 16, 2 * B), F32),
            pltpu.VMEM((hk, 8, 2 * B), F32),
            pltpu.VMEM((hk, 8, 2 * B), F32),
            pltpu.VMEM((2, hk, 8, 2 * B), F32),
            pltpu.VMEM((T, 2 * DH), BF16),
            pltpu.VMEM((5 * T, DH), BF16),
            pltpu.VMEM((T, DH), BF16),
            pltpu.VMEM((T // 2, DH), BF16),
            pltpu.VMEM((2, 8, DH), F32),
            pltpu.VMEM((1, docs), I32),
            sem((3, hk)),
            sem((2, hk)),
            sem((hk,)),
            sem((hk,)),
            sem((hk,)),
            sem((hk,)),
            sem((2, hk)),
            sem((hk,)),
            sem((2, hk)),
            sem((hk,)),
            sem((hk,)),
            sem,
            sem,
            sem,
        ],
        compiler_params=pltpu.CompilerParams(
            collective_id=0, has_side_effects=True, vmem_limit_bytes=36 * 1024 * 1024
        ),
    )(*[pltpu.with_memory_space_constraint(x, pltpu.HBM) for x in (queries, keys, values, doc_lengths.reshape(1, docs))])


def solution(mesh):
    return jax.shard_map(
        on_device,
        mesh=mesh,
        in_specs=(P(("grp", "cp"), None), P(("grp", "cp"), None), P(("grp", "cp"), None), P("grp")),
        out_specs=P(("grp", "cp"), None),
        check_vma=False,
    )
```

```python
import functools
import math

import jax
import jax.numpy as jnp
from jax import lax
from jax.experimental import pallas as pl
from jax.experimental.pallas import tpu as pltpu
from jax.sharding import PartitionSpec as P

DH = 128
T = 512
B = 128
BORDER, NEAR, FAR, WHOLE = 512, (256, 512), 256, 512
LAG = 3
FIRST_LAG, LAST_LAG = 4, 5
LINE = 8
BIG = 32768.0
NEG = -1e30
SCALE = 144.0 ** (-0.5) * math.log2(math.e)
MESH = pl.DeviceIdType.MESH
F32, BF16, I32 = jnp.float32, jnp.bfloat16, jnp.int32


def stacked(pair):
    return jnp.concatenate([pair[:, :DH], pair[:, DH:]], axis=0)


def kernel(
    q_hbm, k_hbm, v_hbm, len_hbm, o_ref,
    kv, qv, qr, raw, msg, held, tops, stat_s, stat_r, early, augk, augq, augr, flags, len_ref,
    loc_sem, q_send, q_recv, own_send, own_recv, msg_send, msg_recv,
    st_send, st_recv, fwd_send, fwd_recv, whole_send, whole_recv, len_sem,
):
    hk = kv.shape[0]
    n = lax.axis_size("cp")
    me = lax.axis_index("cp")
    core = lax.rem(me, 2)
    chip = lax.div(me, 2)
    partner = me + 1 - 2 * core
    next_head = lax.rem(me + 2 - core, n)
    last_head = lax.rem(me + n - 2, n)
    last_tail = lax.rem(me + n - 1, n)
    own0 = pl.multiple_of(T + T * core, T)
    barrier = pltpu.get_barrier_semaphore()
    half = T // 2

    def lanes(h, width):
        return pl.ds(pl.multiple_of(h * width, DH), width)

    def local(h):
        mine = pl.ds(own0, T)
        return (
            pltpu.make_async_copy(k_hbm.at[:, lanes(h, DH)], kv.at[h, mine, pl.ds(0, DH)], loc_sem.at[0, h]),
            pltpu.make_async_copy(v_hbm.at[:, lanes(h, DH)], raw.at[h], loc_sem.at[1, h]),
            pltpu.make_async_copy(q_hbm.at[:, lanes(h, 2 * DH)], qv.at[h], loc_sem.at[2, h]),
        )

    def remote(src, dst, send, recv, to):
        return pltpu.make_async_remote_copy(src, dst, send, recv, device_id={"cp": to}, device_id_type=MESH)

    def send_q(h, part):
        src = qv.at[h, pl.ds(part * half, half)]
        return remote(src, qr.at[h], q_send.at[part, h], q_recv.at[h], (last_head, last_tail)[part])

    def send_own(h):
        mine = kv.at[h, pl.ds(own0, T)]
        return remote(mine, mine, own_send.at[h], own_recv.at[h], partner)

    def send_msg(h, part):
        dst = kv.at[h, pl.ds(part * half, half)]
        return remote(msg.at[h], dst, msg_send.at[h], msg_recv.at[part, h], next_head)

    def send_stat(h, part):
        return remote(stat_s.at[h], stat_r.at[part, h], st_send.at[h], st_recv.at[part, h], next_head)

    def send_whole(part):
        src = kv.at[hk - 1, pl.ds(T + part * T, T)]
        dst = (early, kv.at[hk - 1, pl.ds(0, T)])[part]
        return remote(src, dst, whole_send, (whole_recv, msg_recv.at[0, hk - 1])[part], next_head)

    def forward(h, part):
        rows = kv.at[h, pl.ds(part * half, half)]
        return remote(rows, rows, fwd_send.at[part, h], fwd_recv.at[part, h], partner)

    def every(body):
        def step(h, carry):
            body(h)
            return carry

        lax.fori_loop(0, hk, step, 0)

    def start_local(which):
        def start(h):
            local(h)[which].start()

        return start

    lengths = pltpu.make_async_copy(len_hbm, len_ref, len_sem)
    lengths.start()
    for which in (2, 1, 0):
        every(start_local(which))

    place = lax.rem(chip, LINE)
    lag = jnp.where(place == 0, FIRST_LAG, jnp.where(place == LINE - 1, LAST_LAG, LAG))
    has_left = chip > 0
    has_right = chip < lax.div(n, 2) - 1

    def greet(other):
        pl.semaphore_signal(barrier, inc=1, device_id={"cp": other}, device_id_type=MESH)

    greet(partner)

    @pl.when(has_right)
    def _():
        greet(next_head)

    @pl.when(has_left & (core == 0))
    def _():
        greet(last_head)
        greet(last_tail)

    right, left = jnp.where(has_right, 1, 0), jnp.where(has_left, 1, 0)
    pl.semaphore_wait(barrier, 1 + right + 2 * left * (1 - core))

    def query(h):
        local(h)[2].wait()

        @pl.when(has_left & (core == 0))
        def _():
            @pl.when(h < hk - 1)
            def _():
                send_q(h, 0).start()
                send_q(h, 1).start()

    every(query)

    @pl.when(chip == 0)
    def _():
        def clear(h):
            kv[h, 0:T] = jnp.zeros((T, 2 * DH), BF16)

        every(clear)
        early[...] = jnp.zeros((T, 2 * DH), BF16)

    def turn(h):
        for copy in local(h)[:2]:
            copy.wait()
        for i in range(0, T, DH):
            block = jnp.transpose(raw[h, i : i + DH].astype(F32)).astype(BF16)
            kv[h, pl.ds(pl.multiple_of(own0 + i, DH), DH), DH : 2 * DH] = block

    def share(i, carry):
        @pl.when(i < hk)
        def _():
            turn(lax.rem(i + hk - 1, hk))

        @pl.when(i > 0)
        def _():
            send_own(lax.rem(i + hk - 2, hk)).start()

        @pl.when((i == 1) & has_right)
        def _():
            @pl.when(core == 0)
            def _():
                send_whole(0).start()

            @pl.when(core == 1)
            def _():
                send_whole(1).start()

        return carry

    lax.fori_loop(0, hk + 1, share, 0)

    lengths.wait()
    lens = jnp.broadcast_to(len_ref[...], (8, len_ref.shape[1]))
    docs = lens.shape[1]
    upto = lax.broadcasted_iota(I32, (docs, docs), 0) <= lax.broadcasted_iota(I32, (docs, docs), 1)
    upto = jnp.where(upto, 1.0, 0.0).astype(BF16)
    high = lax.shift_right_logical(lens, 5).astype(F32).astype(BF16)
    low = (lens & 31).astype(F32).astype(BF16)
    ends = 32.0 * jnp.dot(high, upto, preferred_element_type=F32) + jnp.dot(low, upto, preferred_element_type=F32)
    ends = ends[0:1].astype(I32)
    ones = jnp.ones((docs, DH), BF16)

    def doc_of(pos):
        past = jnp.where(pos >= ends, 1.0, 0.0).astype(BF16)
        return jnp.dot(past, ones, preferred_element_type=F32)

    def doc_rows(base, rows):
        return doc_of(lax.broadcasted_iota(I32, (rows, docs), 0) + base)

    def doc_at(p):
        return doc_of(jnp.zeros((8, docs), I32) + p)

    def bits(doc):
        lane = lax.broadcasted_iota(I32, doc.shape, 1)
        return (lax.shift_right_logical(doc.astype(I32), lane & 7) & 1).astype(F32), lane

    def key_side(doc, hidden):
        b, lane = bits(doc)
        out = jnp.where(lane < 8, b - 1.0, jnp.where(lane < 16, -b, jnp.where(lane == 16, -hidden, 0.0)))
        return (out * BIG).astype(BF16)

    def query_side(doc):
        b, lane = bits(doc)
        return jnp.where(lane < 8, b, jnp.where(lane < 16, 1.0 - b, jnp.where(lane == 16, 1.0, 0.0))).astype(BF16)

    first = chip * (2 * T)
    inner = jnp.where(chip > 0, 1.0, 0.0)
    far_left = jnp.where(doc_at(first - T - 1) == doc_at(first), 1.0, 0.0) * inner
    far_right = jnp.where(doc_at(first + T - 1) == doc_at(first + 2 * T), 1.0, 0.0)
    flags[0] = far_left
    flags[1] = far_right
    hidden = jnp.maximum(far_left, 1.0 - inner)[0:1]
    for part in range(3):
        doc = doc_rows(first + (part - 1) * T, T)
        augk[part * T : (part + 1) * T] = key_side(doc, hidden if part == 0 else 0.0)
        if part == 0:
            augk[4 * T : 5 * T] = key_side(doc, 1.0 - inner)
    augk[3 * T : 4 * T] = key_side(doc_rows(first - 2 * T, T), 1.0 - inner)
    augq[...] = query_side(doc_rows(me * T, T))
    augr[...] = query_side(doc_rows(first + 2 * T + core * half, half))

    ones_v = jnp.ones((16, 3 * T), BF16)
    column = lax.broadcasted_iota(I32, (B, 2 * B), 1)
    causal = lax.broadcasted_iota(I32, (B, 2 * B), 0) <= (column & (B - 1))

    def chunks(lo, hi, size):
        if lo < 0 < hi:
            return chunks(lo, 0, size) + chunks(0, hi, size)
        return [(i, min(i + size, hi)) for i in range(lo, hi, size)]

    def rows_of(h, i, j):
        return early[i + T : j + T] if i < 0 else kv[h, i:j]

    def aug_of(i, j, last):
        return augk[i + 4 * T : j + 4 * T] if last and j <= T else augk[i:j]

    def scores(h, pair, aug, lo, hi, size, diagonal, last=False):
        q = jnp.concatenate([stacked(pair), jnp.concatenate([aug, aug], axis=0)], axis=1)
        found, top = [], None
        for i, j in chunks(lo, hi, size):
            k = jnp.concatenate([rows_of(h, i, j)[:, 0:DH], aug_of(i, j, last)], axis=1)
            s = lax.dot_general(k, q, (((1,), (1,)), ((), ())), preferred_element_type=F32)
            if diagonal and j == hi:
                end = jnp.where(causal, s[-B:], NEG)
                s = jnp.concatenate([s[:-B], end], axis=0) if j - i > B else end
            high = jnp.max(s, axis=0, keepdims=True)
            top = high if top is None else jnp.maximum(top, high)
            found.append(s)
            yield
        return found, top * SCALE

    def mixed(h, found, top, lo, hi, size):
        o = None
        for s, (i, j) in zip(found, chunks(lo, hi, size)):
            p = jnp.exp2(s * SCALE - top).astype(BF16)
            v = jnp.concatenate([rows_of(h, k, k + B)[:, DH : 2 * DH] for k in range(i, j, B)], axis=1)
            v = jnp.concatenate([v, ones_v[:, : j - i]], axis=0)
            part = jnp.dot(v, p, preferred_element_type=F32)
            o = part if o is None else o + part
            yield
        return o

    def store(h, r, o):
        rows = slice(r * B, (r + 1) * B)
        o_ref[rows, lanes(2 * h, DH)] = jnp.transpose(o[:, :B]).astype(BF16)
        o_ref[rows, lanes(2 * h + 1, DH)] = jnp.transpose(o[:, B:]).astype(BF16)

    def staggered(blocks):
        behind = []
        for block in [*blocks, None, None]:
            if block is not None:
                for _ in iter(lambda: next(block), "scored"):
                    if len(behind) > 1:
                        next(behind[0], None)
            if len(behind) > 1 or (block is None and behind):
                for _ in behind.pop(0):
                    pass
            if block is not None:
                behind.append(block)

    def border_block(h, i, part):
        rows = slice(i * B, (i + 1) * B)
        r = part * 2 + i
        lo, hi = T + r * B, 3 * T
        s, top = yield from scores(h, qr[h, rows], augr[rows], lo, hi, BORDER, False)
        yield "scored"
        o = yield from mixed(h, s, top, lo, hi, BORDER)
        acc, total = o[:DH], o[DH : DH + 1]
        own = kv[h, 2 * T + r * B : 2 * T + (r + 1) * B].astype(F32)
        msg[h, rows] = jnp.where(flags[1][0:1, 0:1] > 0.5, acc / total, own).astype(BF16)
        stat_s[h, :, i * 2 * B : (i + 1) * 2 * B] = top + jnp.log2(total)

    def border(h, part):
        send_q(h, part).wait_recv()
        staggered(border_block(h, i, part) for i in range(2))
        send_msg(h, part).start()
        send_stat(h, part).start()

    def near_block(h, r, core):
        rows = slice(r * B, (r + 1) * B)
        lo, hi = T, T + core * T + (r + 1) * B
        s, top = yield from scores(h, qv[h, rows], augq[rows], lo, hi, NEAR[core], True)
        yield "scored"
        held[h, r] = yield from mixed(h, s, top, lo, hi, NEAR[core])
        tops[h, r : r + 1] = top

    def far_block(h, r, core, last=False):
        rows = slice(r * B, (r + 1) * B)
        lo, hi, size = core * r * B, T, WHOLE if last else FAR
        if last and core == 0:
            lo = r * B - T
        s, top = yield from scores(h, qv[h, rows], augq[rows], lo, hi, size, False, last)
        yield "scored"
        before = tops[h, r : r + 1]
        top = jnp.maximum(top, before)
        if core == 0 and not last:
            i = r % 2 * 2 * B
            level = jnp.where(flags[0][0:1, 0:1] > 0.5, stat_r[r // 2, h, :, i : i + 2 * B], NEG)
            top = jnp.maximum(top, level)
        o = yield from mixed(h, s, top, lo, hi, size)
        o = o + held[h, r] * jnp.exp2(before - top)
        acc, total = o[:DH], o[DH : DH + 1]
        if core == 0 and not last:
            weight = jnp.exp2(level - top)
            acc, total = acc + weight * kv[h, rows].astype(F32), total + weight
        store(h, r, acc / total)

    @pl.when(core == 0)
    def _():
        def step(it, carry):
            h = it - lag

            @pl.when((it >= lag) & (h < hk - 1) & has_left)
            def _():
                for part in range(2):
                    send_msg(h, part).wait_recv()
                    forward(h, part).start()
                for part in range(2):
                    send_stat(h, part).wait_recv()

            @pl.when((it == min(4, hk - 1)) & has_left)
            def _():
                send_whole(1).wait_recv()
                for part in range(2):
                    forward(hk - 1, part).start()

            @pl.when(it < hk)
            def _():
                send_own(it).wait_recv()

                @pl.when(has_right & (it < hk - 1))
                def _():
                    border(it, 0)

                staggered(near_block(it, r, 0) for r in reversed(range(T // B)))

            @pl.when((it >= lag) & (h < hk - 1))
            def _():
                staggered(far_block(h, r, 0) for r in range(T // B))

            @pl.when(it == hk - 1)
            def _():
                @pl.when(has_left)
                def _():
                    send_whole(0).wait_recv()

                staggered(far_block(hk - 1, r, 0, True) for r in range(T // B))

            return carry

        lax.fori_loop(0, hk + max(FIRST_LAG, LAST_LAG) - 1, step, 0)

        def finish(h):
            send_own(h).wait_send()

            @pl.when(has_left)
            def _():
                for part in range(2):
                    forward(h, part).wait_send()

            @pl.when(has_left & (h < hk - 1))
            def _():
                for part in range(2):
                    send_q(h, part).wait_send()

            @pl.when(has_right & (h < hk - 1))
            def _():
                send_msg(h, 0).wait_send()
                send_stat(h, 0).wait_send()

            @pl.when(has_right & (h == hk - 1))
            def _():
                send_whole(0).wait_send()

        every(finish)

    @pl.when(core == 1)
    def _():
        def step(it, carry):
            h = it - lag

            @pl.when(it < hk)
            def _():
                send_own(it).wait_recv()

                @pl.when(has_right & (it < hk - 1))
                def _():
                    border(it, 1)

                staggered(near_block(it, r, 1) for r in reversed(range(T // B)))

            @pl.when((it >= lag) & (h < hk - 1))
            def _():
                @pl.when(has_left)
                def _():
                    for part in range(2):
                        forward(h, part).wait_recv()

                staggered(far_block(h, r, 1) for r in range(T // B))

            @pl.when(it == hk - 1)
            def _():
                @pl.when(has_left)
                def _():
                    for part in range(2):
                        forward(hk - 1, part).wait_recv()

                staggered(far_block(hk - 1, r, 1, True) for r in range(T // B))

            return carry

        lax.fori_loop(0, hk + max(FIRST_LAG, LAST_LAG) - 1, step, 0)

        def finish(h):
            send_own(h).wait_send()

            @pl.when(has_right & (h < hk - 1))
            def _():
                send_msg(h, 1).wait_send()
                send_stat(h, 1).wait_send()

            @pl.when(has_right & (h == hk - 1))
            def _():
                send_whole(1).wait_send()

        every(finish)


def on_device(queries, keys, values, doc_lengths):
    hk = keys.shape[1] // DH
    docs = doc_lengths.shape[0]
    sem = pltpu.SemaphoreType.DMA
    hbm = pl.BlockSpec(memory_space=pltpu.HBM)
    vmem = pl.BlockSpec(memory_space=pltpu.VMEM)
    return pl.pallas_call(
        kernel,
        out_shape=pltpu.VMEM(queries.shape, BF16),
        in_specs=[hbm, hbm, hbm, hbm],
        out_specs=vmem,
        scratch_shapes=[
            pltpu.VMEM((hk, 3 * T, 2 * DH), BF16),
            pltpu.VMEM((hk, T, 2 * DH), BF16),
            pltpu.VMEM((hk, T // 2, 2 * DH), BF16),
            pltpu.VMEM((hk, T, DH), BF16),
            pltpu.VMEM((hk, T // 2, 2 * DH), BF16),
            pltpu.VMEM((hk, T // B, DH + 16, 2 * B), F32),
            pltpu.VMEM((hk, 8, 2 * B), F32),
            pltpu.VMEM((hk, 1, 4 * B), F32),
            pltpu.VMEM((2, hk, 1, 4 * B), F32),
            pltpu.VMEM((T, 2 * DH), BF16),
            pltpu.VMEM((5 * T, DH), BF16),
            pltpu.VMEM((T, DH), BF16),
            pltpu.VMEM((T // 2, DH), BF16),
            pltpu.VMEM((2, 8, DH), F32),
            pltpu.VMEM((1, docs), I32),
            sem((3, hk)),
            sem((2, hk)),
            sem((hk,)),
            sem((hk,)),
            sem((hk,)),
            sem((hk,)),
            sem((2, hk)),
            sem((hk,)),
            sem((2, hk)),
            sem((2, hk)),
            sem((2, hk)),
            sem,
            sem,
            sem,
        ],
        compiler_params=pltpu.CompilerParams(
            collective_id=0, has_side_effects=True, vmem_limit_bytes=36 * 1024 * 1024
        ),
    )(*[pltpu.with_memory_space_constraint(x, pltpu.HBM) for x in (queries, keys, values, doc_lengths.reshape(1, docs))])


def solution(mesh):
    return jax.shard_map(
        on_device,
        mesh=mesh,
        in_specs=(P(("grp", "cp"), None), P(("grp", "cp"), None), P(("grp", "cp"), None), P("grp")),
        out_specs=P(("grp", "cp"), None),
        check_vma=False,
    )
```
